256 devices in a mesh: sx: 16 (over y_hi, z), sy: 16 (over x, y_lo, core).
Axes of the slice: x: 4, y: 4 (y_hi: 2, y_lo: 2; y = y_hi * 2 + y_lo), z: 8, core: 2. Of those that a mesh axis runs over, the one named last changes fastest.
Arguments:
- tensors: bfloat16 [2, 16, 16, 1024, 256], P(None, 'sx', 'sy'), may hold values from -6 to 6
- gates: bfloat16 [8, 2, 2, 256, 256], replicated, may hold values from -0.1875 to 0.1875
- closing_rows: bfloat16 [2, 4096, 1024], P(None, ('sx', 'sy')), may hold values from -0.125 to 0.125
- closing_columns: float32 [2, 4096, 256], P(None, ('sx', 'sy')), may hold values from -0.25 to 0.25
Outputs:
- amplitudes: float32 [2, 4096], replicated
The draws below stay inside these ranges and needn't reach their ends.
All inputs are finite; a program needn't handle non-finite values.
Results may differ from the reference program's by a relative error of at most 0.012.
Values may be sent and summed in bfloat16 or wider, within the bound.
A program may use at most 64 MiB of HBM per device.

```python
import jax
import jax.numpy as jnp
from jax import lax

C = 256
R = 1024
AMPS = 4096
BX = 4
SECTIONS = 8
AMP_DEV = 16
N_SX = 16
N_SY = 16


def shard_levels(stream_key, dims, pieces, smallest, largest):
    factor_of = 1.0
    for position, parts in pieces:
        heights = jax.random.uniform(jax.random.fold_in(jax.random.fold_in(stream_key, 6), position), (parts,), jnp.float32, smallest / len(pieces), largest / len(pieces))
        factor_of = factor_of * jnp.repeat(jnp.exp(heights), dims[position] // parts).reshape((-1,) + (1,) * (len(dims) - 1 - position))
    return factor_of


def scatter_about(stream_key, shape, deviation, limit, cuts=(), dtype=jnp.bfloat16):
    level = shard_levels(stream_key, shape, cuts, -0.22, 0.18) if cuts else 1.0
    entries = jax.random.normal(stream_key, shape, jnp.float32) * deviation * level
    return jnp.minimum(jnp.maximum(entries, -limit), limit).astype(dtype)


def setup_inputs(seed: int = 0) -> dict:
    key_of = jax.random.split(jax.random.key(seed), 5)
    return {
        "tensors": scatter_about(key_of[0], (2, N_SX, N_SY, R, C), 1.0, 6.0, ((1, 16), (2, 16))),
        "gates": scatter_about(key_of[1], (SECTIONS, 2, 2, C, C), (4 * C) ** -0.5, 0.1875),
        "closing_rows": scatter_about(key_of[2], (2, AMPS, R), (2 * R) ** -0.5, 0.125, ((1, 256),)),
        "closing_columns": scatter_about(key_of[3], (2, AMPS, C), (2 * C) ** -0.5, 0.25, ((1, 256),), jnp.float32),
    }


HIGH = lax.Precision.HIGHEST


def complex_product(values, matrix):
    values = values.astype(jnp.float32)
    matrix = matrix.astype(jnp.float32)
    real_part = jnp.matmul(values[0], matrix[0], precision=HIGH) - jnp.matmul(values[1], matrix[1], precision=HIGH)
    imag_part = jnp.matmul(values[0], matrix[1], precision=HIGH) + jnp.matmul(values[1], matrix[0], precision=HIGH)
    return jnp.stack([real_part, imag_part])


def apply_section(current, gate_pair, axis_dim, bit_pos):
    shape = current.shape
    count = shape[axis_dim]
    split = shape[:axis_dim] + (count >> (bit_pos + 1), 2, 1 << bit_pos) + shape[axis_dim + 1:]
    blocks = current.reshape(split)
    lower = jnp.take(blocks, 0, axis=axis_dim + 1)
    upper = jnp.take(blocks, 1, axis=axis_dim + 1)
    new_lower = complex_product(lower, gate_pair[0]) + complex_product(upper, gate_pair[1])
    new_upper = complex_product(upper, gate_pair[0]) - complex_product(lower, gate_pair[1])
    joined = jnp.stack([new_lower, new_upper], axis=axis_dim + 1).reshape(shape)
    return joined.astype(jnp.bfloat16)


def reference(tensors, gates, closing_rows, closing_columns):
    current = tensors
    for number in range(SECTIONS):
        if number < BX:
            current = apply_section(current, gates[number], 1, number)
        else:
            current = apply_section(current, gates[number], 2, number - BX)
    slices = N_SX * N_SY
    flat = current.reshape(2, slices, R, C).astype(jnp.float32)
    row_close = closing_rows.reshape(2, slices, AMP_DEV, R).astype(jnp.float32)
    column_close = closing_columns.reshape(2, slices, AMP_DEV, C)
    proj_real = jnp.matmul(row_close[0], flat[0], precision=HIGH) - jnp.matmul(row_close[1], flat[1], precision=HIGH)
    proj_imag = jnp.matmul(row_close[0], flat[1], precision=HIGH) + jnp.matmul(row_close[1], flat[0], precision=HIGH)
    amp_real = jnp.sum(proj_real * column_close[0] - proj_imag * column_close[1], axis=-1)
    amp_imag = jnp.sum(proj_real * column_close[1] + proj_imag * column_close[0], axis=-1)
    return jnp.stack([amp_real, amp_imag]).reshape(2, AMPS)
```

```python
import functools

import jax
import jax.numpy as jnp
from jax import lax
from jax.experimental import pallas as pl
from jax.experimental.pallas import tpu as pltpu
from jax.sharding import PartitionSpec as P

MESH = pl.DeviceIdType.MESH


def gather_kernel(count_x, count_y, own_ref, out_ref, send_x, recv_x, send_y, recv_y):
    sx = lax.axis_index("sx")
    sy = lax.axis_index("sy")
    barrier = pltpu.get_barrier_semaphore()
    for step in range(1, count_x):
        peer = lax.rem(sx + step, count_x)
        pl.semaphore_signal(barrier, inc=1, device_id=(peer, sy), device_id_type=MESH)
    for step in range(1, count_y):
        peer = lax.rem(sy + step, count_y)
        pl.semaphore_signal(barrier, inc=1, device_id=(sx, peer), device_id_type=MESH)
    pl.semaphore_wait(barrier, count_x + count_y - 2)
    copies = []
    for step in range(1, count_x):
        copy = pltpu.make_async_remote_copy(
            src_ref=own_ref,
            dst_ref=out_ref.at[sy, sx],
            send_sem=send_x.at[step - 1],
            recv_sem=recv_x.at[step - 1],
            device_id=(lax.rem(sx + step, count_x), sy),
            device_id_type=MESH,
        )
        copy.start()
        copies.append(copy)
    out_ref[sy, sx] = own_ref[...]
    for copy in copies:
        copy.wait()
    copies = []
    for step in range(1, count_y):
        copy = pltpu.make_async_remote_copy(
            src_ref=out_ref.at[sy],
            dst_ref=out_ref.at[sy],
            send_sem=send_y.at[step - 1],
            recv_sem=recv_y.at[step - 1],
            device_id=(sx, lax.rem(sy + step, count_y)),
            device_id_type=MESH,
        )
        copy.start()
        copies.append(copy)
    for copy in copies:
        copy.wait()


def gather_amplitudes(closed, count_x, count_y):
    amps = closed.shape[1]
    row = jnp.concatenate([closed.reshape(1, 2 * amps), jnp.zeros((1, 128 - 2 * amps), jnp.float32)], axis=1)
    rows = pl.pallas_call(
        functools.partial(gather_kernel, count_x, count_y),
        out_shape=jax.ShapeDtypeStruct((count_y, count_x, 1, 128), jnp.float32),
        in_specs=[pl.BlockSpec(memory_space=pltpu.VMEM)],
        out_specs=pl.BlockSpec(memory_space=pltpu.VMEM),
        scratch_shapes=[
            pltpu.SemaphoreType.DMA((count_x - 1,)),
            pltpu.SemaphoreType.DMA((count_x - 1,)),
            pltpu.SemaphoreType.DMA((count_y - 1,)),
            pltpu.SemaphoreType.DMA((count_y - 1,)),
        ],
        compiler_params=pltpu.CompilerParams(collective_id=0, has_side_effects=True),
        name="gather",
    )(row)
    rows = rows[:, :, 0, : 2 * amps].reshape(count_y, count_x, 2, amps)
    return rows.transpose(2, 1, 0, 3).reshape(2, count_x * count_y * amps)


def mixing_matrix(gate_pair, sign):
    own_top = jnp.concatenate([gate_pair[0, 0], gate_pair[0, 1]], axis=1)
    own_low = jnp.concatenate([-gate_pair[0, 1], gate_pair[0, 0]], axis=1)
    far_top = jnp.concatenate([gate_pair[1, 0], gate_pair[1, 1]], axis=1) * sign
    far_low = jnp.concatenate([-gate_pair[1, 1], gate_pair[1, 0]], axis=1) * sign
    return jnp.concatenate([own_top, own_low, far_top, far_low], axis=0)


def combine(own, partner, matrix):
    width = own.shape[-1]
    leading = own.shape[1:-1]
    joined = jnp.concatenate([own[0], own[1], partner[0], partner[1]], axis=-1).reshape(
        -1, 4 * width
    )
    result = jnp.dot(joined, matrix, preferred_element_type=jnp.float32).astype(jnp.bfloat16)
    real_part = result[:, :width].reshape(leading + (width,))
    imag_part = result[:, width:].reshape(leading + (width,))
    return jnp.stack([real_part, imag_part])


def local_section(grouped, gate_pair, axis_dim, bit_pos):
    shape = grouped.shape
    count = shape[axis_dim]
    split = shape[:axis_dim] + (count >> bit_pos + 1, 2, 1 << bit_pos) + shape[axis_dim + 1 :]
    blocks = grouped.reshape(split)
    lower = lax.index_in_dim(blocks, 0, axis_dim + 1, keepdims=False)
    upper = lax.index_in_dim(blocks, 1, axis_dim + 1, keepdims=False)
    new_lower = combine(lower, upper, mixing_matrix(gate_pair, 1.0))
    new_upper = combine(upper, lower, mixing_matrix(gate_pair, -1.0))
    return jnp.stack([new_lower, new_upper], axis=axis_dim + 1).reshape(shape)


def close_columns(projected, closing_columns):
    amp_real = jnp.sum(
        projected[0] * closing_columns[0] - projected[1] * closing_columns[1], axis=-1
    )
    amp_imag = jnp.sum(
        projected[0] * closing_columns[1] + projected[1] * closing_columns[0], axis=-1
    )
    return jnp.stack([amp_real, amp_imag])


def combine_rows(closing_rows, current):
    proj_real = jnp.dot(closing_rows[0], current[0], preferred_element_type=jnp.float32) - jnp.dot(
        closing_rows[1], current[1], preferred_element_type=jnp.float32
    )
    proj_imag = jnp.dot(closing_rows[0], current[1], preferred_element_type=jnp.float32) + jnp.dot(
        closing_rows[1], current[0], preferred_element_type=jnp.float32
    )
    return jnp.stack([proj_real, proj_imag])


def local(tensors, gates, closing_rows, closing_columns):
    current = tensors[:, 0, 0]
    rows_dev = current.shape[1]
    width = current.shape[2]
    count_x = lax.axis_size("sx")
    count_y = lax.axis_size("sy")
    bits_x = count_x.bit_length() - 1
    bits_y = count_y.bit_length() - 1
    grouped = lax.all_to_all(
        current.reshape(2, count_x, rows_dev // count_x, width),
        "sx",
        split_axis=1,
        concat_axis=1,
        tiled=True,
    )
    for bit_pos in range(bits_x):
        grouped = local_section(grouped, gates[bit_pos], 1, bit_pos)
    current = lax.all_to_all(grouped, "sx", split_axis=1, concat_axis=1, tiled=True).reshape(
        2, rows_dev, width
    )
    grouped = lax.all_to_all(
        current.reshape(2, count_y, rows_dev // count_y, width),
        "sy",
        split_axis=1,
        concat_axis=1,
        tiled=True,
    )
    for bit_pos in range(bits_y):
        grouped = local_section(grouped, gates[bits_x + bit_pos], 1, bit_pos)
    current = lax.all_to_all(grouped, "sy", split_axis=1, concat_axis=1, tiled=True).reshape(
        2, rows_dev, width
    )
    closed = close_columns(combine_rows(closing_rows, current), closing_columns)
    return gather_amplitudes(closed, count_x, count_y)


def solution(mesh):
    placed = (
        P(None, "sx", "sy", None, None),
        P(),
        P(None, ("sx", "sy"), None),
        P(None, ("sx", "sy"), None),
    )
    return jax.shard_map(local, mesh=mesh, in_specs=placed, out_specs=P(), check_vma=False)
```

```python
import functools

import jax
import jax.numpy as jnp
from jax import lax
from jax.experimental import pallas as pl
from jax.experimental.pallas import tpu as pltpu
from jax.sharding import PartitionSpec as P

MESH = pl.DeviceIdType.MESH
F32 = jnp.float32
BF16 = jnp.bfloat16
NZ, NY, NX, NC = 8, 4, 4, 2
NH = NY * NC
GROUP = NZ * NH
C = 256
CHUNKS = 2
KR = 16 // CHUNKS
AMP = 16
Z_ORDER = (4, 3, 5, 2, 6, 1, 7, 0)
Y_ORDER = (2, 1, 3, 0)


def position():
    sx = lax.axis_index("sx")
    sy = lax.axis_index("sy")
    return lax.rem(sx, 8), (sx // 8) * 2 + lax.rem(sy // 2, 2), sy // 4, lax.rem(sy, 2)


def device(z, y, x, c):
    return ((y // 2) * 8 + z, x * 4 + lax.rem(y, 2) * 2 + c)


def bits_index(y, c):
    return y // 2 + 2 * c + 4 * lax.rem(y, 2)


def ones(number):
    return bin(number).count("1")


def turned(block, power):
    power %= 4
    re, im = block[:, :C], block[:, C:]
    if power == 0:
        return block
    if power == 1:
        return jnp.concatenate([-im, re], axis=1)
    if power == 2:
        return -block
    return jnp.concatenate([im, -re], axis=1)


def hadamard(blocks):
    blocks = list(blocks)
    half = 1
    while half < len(blocks):
        for low in range(len(blocks)):
            if not low & half:
                a, b = blocks[low], blocks[low | half]
                blocks[low], blocks[low | half] = a + b, a - b
        half *= 2
    return blocks


def fill_full(full, index, re, im):
    full[index, :C, :C] = re
    full[index, :C, C:] = im
    full[index, C:, :C] = -im
    full[index, C:, C:] = re


def section_pairs(gates, first, right, tops):
    for which in range(2):
        tops[which, :, :C] = gates[first, which, 0]
        tops[which, :, C:] = gates[first, which, 1]
        fill_full(right, which, gates[first + 1, which, 0], gates[first + 1, which, 1])
    aa = jnp.dot(tops[0], right[0], preferred_element_type=F32)
    bb = jnp.dot(tops[1], right[1], preferred_element_type=F32)
    even, odd = aa - bb, aa + bb
    ba = jnp.dot(tops[1], right[0], preferred_element_type=F32)
    ab = jnp.dot(tops[0], right[1], preferred_element_type=F32)
    plus, minus = turned(ba + ab, -1), turned(ba - ab, -1)
    return even + plus, odd - minus, odd + minus, even - plus


def triple_products(gates, first, right, tops, full):
    for low, pair in enumerate(section_pairs(gates, first, right, tops)):
        tops[2 + low] = pair.astype(BF16)
    for which in range(2):
        fill_full(right, which, gates[first + 2, which, 0], gates[first + 2, which, 1])
    for low in range(4):
        with_a = jnp.dot(tops[2 + low], right[0], preferred_element_type=F32)
        with_b = turned(jnp.dot(tops[2 + low], right[1], preferred_element_type=F32), -1)
        for third, out in enumerate((with_a + with_b, with_a - with_b)):
            out = out.astype(BF16)
            fill_full(full, low + 4 * third, out[:, :C], out[:, C:])


def pair_products(gates, first, right, tops, full):
    for low, pair in enumerate(section_pairs(gates, first, right, tops)):
        pair = pair.astype(BF16)
        fill_full(full, low, pair[:, :C], pair[:, C:])


def wait_bytes(ref, sem):
    pltpu.make_async_copy(ref, ref, sem).wait()


def sections(q, recv, work1, work2, g_low, g_high, ret_send):
    def forward_z(h, carry):
        blocks = []
        for z in range(NZ):
            both = recv[q, h * NZ + z].astype(F32)
            blocks.append(turned(jnp.concatenate([both[0], both[1]], axis=1), ones(z)))
        for t, block in enumerate(hadamard(blocks)):
            work1[h, t] = block
        return carry

    def forward_h(t, carry):
        blocks = hadamard([turned(work1[h, t], ones(h)) for h in range(NH)])
        left = jnp.concatenate(blocks, axis=0).astype(BF16)
        out = jnp.dot(left, g_low[t], preferred_element_type=F32)
        for h in range(NH):
            work2[h, t] = out[h * KR : (h + 1) * KR]
        return carry

    def inverse_z(h, carry):
        left = work2[h].reshape(NZ * KR, 2 * C).astype(BF16)
        out = jnp.dot(left, g_high[h], preferred_element_type=F32)
        blocks = hadamard([out[t * KR : (t + 1) * KR] for t in range(NZ)])
        for z in range(NZ):
            work1[h, z] = turned(blocks[z], -ones(z))
        return carry

    def inverse_h(z, carry):
        blocks = hadamard([work1[t, z] for t in range(NH)])
        for h in range(NH):
            ret_send[q, h, z] = (turned(blocks[h], -ones(h)) * (1.0 / GROUP)).astype(BF16)
        return carry

    lax.fori_loop(0, NH, forward_z, 0)
    lax.fori_loop(0, NZ, forward_h, 0)
    lax.fori_loop(0, NH, inverse_z, 0)
    lax.fori_loop(0, NZ, inverse_h, 0)


def kernel(
    x_ref, gates_ref, rows_ref, cols_ref, out_ref,
    recv, work1, work2, ret_send, ret, gates, right, tops, g_low, g_high, g_x,
    cols, crx, ccx, wbuf, finz, finx,
    local_sem, main_send, main_recv, small_send, small_recv, x_send, x_recv, back_send, back_recv, fin_send, fin_recv,
):
    mz, my, mx, mc = position()
    mh = bits_index(my, mc)
    mine = mh * NZ + mz

    z_peers = [lax.rem(mz + d, NZ) for d in range(NZ)]
    y_peers = [lax.rem(my + d, NY) for d in range(NY)]
    c_peers = [lax.rem(mc + d, NC) for d in range(NC)]
    x_peers = [lax.rem(mx + d, NX) for d in range(NX)]
    group = [(dz, dy, dc) for dz in Z_ORDER for dy in Y_ORDER for dc in range(NC) if dz or dy or dc]
    back = [(dy, dc) for dy in Y_ORDER for dc in range(NC) if dy or dc]

    barrier = pltpu.get_barrier_semaphore()
    for dz, dy, dc in group:
        pl.semaphore_signal(barrier, inc=1, device_id=device(z_peers[dz], y_peers[dy], mx, c_peers[dc]), device_id_type=MESH)
    for dx in range(1, NX):
        pl.semaphore_signal(barrier, inc=1, device_id=device(mz, my, x_peers[dx], mc), device_id_type=MESH)

    gates_copy = pltpu.make_async_copy(gates_ref, gates, local_sem.at[0])
    gates_copy.start()
    cols_copy = pltpu.make_async_copy(cols_ref, cols, local_sem.at[1])
    cols_copy.start()
    own_rows = pltpu.make_async_copy(rows_ref.at[:, :, pl.ds(pl.multiple_of(mz * 128, 128), 128)], crx.at[mx, mz], local_sem.at[2])
    own_rows.start()
    own = []
    for q in range(CHUNKS):
        copy = pltpu.make_async_copy(x_ref.at[:, mz * NH + mh, q], recv.at[q, mine], local_sem.at[3 + q])
        copy.start()
        own.append(copy)
    cols_copy.wait()
    ccx[mx, mz] = cols[...].astype(BF16)
    gates_copy.wait()
    triple_products(gates, 0, right, tops, g_low)
    pl.semaphore_wait(barrier, GROUP - 1 + NX - 1)

    def remote(src, dst, send, recv_sem, where):
        copy = pltpu.make_async_remote_copy(
            src_ref=src, dst_ref=dst, send_sem=send, recv_sem=recv_sem, device_id=device(*where), device_id_type=MESH
        )
        copy.start()

    for dz in Z_ORDER[:-1]:
        pz = z_peers[dz]
        there = (pz, my, mx, mc)
        columns = pl.ds(pl.multiple_of(pz * 128, 128), 128)
        remote(rows_ref.at[:, :, columns], crx.at[mx, mz], small_send.at[0], small_recv.at[0], there)
        remote(ccx.at[mx, mz], ccx.at[mx, mz], small_send.at[1], small_recv.at[1], there)
    for q in range(CHUNKS):
        for dz, dy, dc in group:
            pz, py, pc = z_peers[dz], y_peers[dy], c_peers[dc]
            block = pz * NH + bits_index(py, pc)
            remote(x_ref.at[:, block, q], recv.at[q, mine], main_send.at[q], main_recv.at[q], (pz, py, mx, pc))

    triple_products(gates, 3, right, tops, g_high)
    pair_products(gates, 6, right, tops, g_x)

    own_rows.wait()
    wait_bytes(crx.at[0, pl.ds(0, NZ - 1)], small_recv.at[0])
    wait_bytes(ccx.at[0, pl.ds(0, NZ - 1)], small_recv.at[1])
    for dx in (2, 1, 3):
        there = (mz, my, x_peers[dx], mc)
        remote(crx.at[mx], crx.at[mx], x_send.at[0], x_recv.at[0], there)
        remote(ccx.at[mx], ccx.at[mx], x_send.at[1], x_recv.at[1], there)

    def columns_through_x():
        m0, m1 = lax.rem(mx, 2), mx // 2
        for xs in range(NX):
            parts = []
            for z in range(NZ):
                both = ccx[xs, z]
                parts.append(jnp.concatenate([both[0], -both[1]], axis=1))
            left = jnp.concatenate(parts, axis=0)
            s0, s1 = xs % 2, xs // 2
            e0 = s0 + m0 - 2 * s0 * m0
            e1 = s1 + m1 - 2 * s1 * m1
            f0 = (1 - 2 * e0).astype(F32)
            f1 = (1 - 2 * e1).astype(F32)
            turn = lax.rem(m0 + m1 - s0 - s1 + 4, 4)
            odd = lax.rem(turn, 2)
            cos = ((1 - odd) * (1 - turn)).astype(F32)
            sin = (odd * (2 - turn)).astype(F32)
            total = None
            for t in range(4):
                u = lax.dot_general(left, g_x[t], (((1,), (1,)), ((), ())), preferred_element_type=F32)
                if t & 1:
                    u = u * f0
                if t & 2:
                    u = u * f1
                total = u if total is None else total + u
            total = total * 0.25
            re, neg_im = total[:, :C], total[:, C:]
            new_re = cos * re + sin * neg_im
            new_neg = cos * neg_im - sin * re
            for z in range(NZ):
                wbuf[z, xs * AMP : (xs + 1) * AMP, :C] = new_re[z * AMP : (z + 1) * AMP]
                wbuf[z, xs * AMP : (xs + 1) * AMP, C:] = new_neg[z * AMP : (z + 1) * AMP]

    for q in range(CHUNKS):
        own[q].wait()
        wait_bytes(recv.at[q, pl.ds(0, GROUP - 1)], main_recv.at[q])
        sections(q, recv, work1, work2, g_low, g_high, ret_send)
        for dy, dc in back:
            py, pc = y_peers[dy], c_peers[dc]
            remote(ret_send.at[q, bits_index(py, pc)], ret.at[q, mh], back_send.at[q], back_recv.at[q], (mz, py, mx, pc))
        ret[q, mh] = ret_send[q, mh]
        if q == 0:
            wait_bytes(crx.at[pl.ds(0, NX - 1)], x_recv.at[0])
            wait_bytes(ccx.at[pl.ds(0, NX - 1)], x_recv.at[1])
            columns_through_x()

    for q in range(CHUNKS):
        wait_bytes(ret.at[q, pl.ds(0, NH - 1)], back_recv.at[q])

    def close(z, carry):
        blocks = []
        for h in range(NH):
            for q in range(CHUNKS):
                blocks.append(ret[q, h, z].astype(F32))
        tensor = jnp.concatenate(blocks, axis=0).astype(BF16)
        rows = []
        for part in range(2):
            for xs in range(NX):
                rows.append(crx[xs, z, part])
        proj = jnp.dot(jnp.concatenate(rows, axis=0), tensor, preferred_element_type=F32)
        half = NX * AMP
        p_re = proj[:half, :C] - proj[half:, C:]
        p_im = proj[:half, C:] + proj[half:, :C]
        w = wbuf[z]
        w_re, w_neg = w[:, :C], w[:, C:]
        a_re = p_re * w_re + p_im * w_neg
        a_im = p_im * w_re - p_re * w_neg
        both = jnp.concatenate([a_re[:, :128] + a_re[:, 128:], a_im[:, :128] + a_im[:, 128:]], axis=0)
        finz[mz, pl.ds(z, 1)] = jnp.sum(jnp.transpose(both), axis=0, keepdims=True)
        return carry

    lax.fori_loop(0, NZ, close, 0)

    wait_bytes(crx.at[0, pl.ds(0, NZ - 1)], small_send.at[0])
    wait_bytes(ccx.at[0, pl.ds(0, NZ - 1)], small_send.at[1])
    wait_bytes(crx.at[pl.ds(0, NX - 1)], x_send.at[0])
    wait_bytes(ccx.at[pl.ds(0, NX - 1)], x_send.at[1])
    for q in range(CHUNKS):
        wait_bytes(recv.at[q, pl.ds(0, GROUP - 1)], main_send.at[q])
        wait_bytes(ret.at[q, pl.ds(0, NH - 1)], back_send.at[q])

    for dz in Z_ORDER[:-1]:
        remote(finz.at[mz], finz.at[mz], fin_send.at[0], fin_recv.at[0], (z_peers[dz], my, mx, mc))
    wait_bytes(finz.at[pl.ds(0, NZ - 1)], fin_recv.at[0])
    finx[mx] = jnp.sum(finz[...], axis=0)
    wait_bytes(finz.at[pl.ds(0, NZ - 1)], fin_send.at[0])
    for dx in (2, 1, 3):
        remote(finx.at[mx], finx.at[mx], fin_send.at[1], fin_recv.at[1], (mz, my, x_peers[dx], mc))
    wait_bytes(finx.at[pl.ds(0, NX - 1)], fin_recv.at[1])
    out_ref[mh] = jnp.sum(finx[...], axis=0)
    wait_bytes(finx.at[pl.ds(0, NX - 1)], fin_send.at[1])
    for dy, dc in back:
        remote(out_ref.at[mh], out_ref.at[mh], fin_send.at[2], fin_recv.at[2], (mz, y_peers[dy], mx, c_peers[dc]))
    wait_bytes(out_ref.at[pl.ds(0, NH - 1)], fin_recv.at[2])
    wait_bytes(out_ref.at[pl.ds(0, NH - 1)], fin_send.at[2])


def local(tensors, gates, closing_rows, closing_columns):
    dma = pltpu.SemaphoreType.DMA
    out = pl.pallas_call(
        kernel,
        out_shape=jax.ShapeDtypeStruct((NH, NZ, 128), F32),
        in_specs=[pl.BlockSpec(memory_space=pl.ANY)] * 4,
        out_specs=pl.BlockSpec(memory_space=pltpu.VMEM),
        scratch_shapes=[
            pltpu.VMEM((CHUNKS, GROUP, 2, KR, C), BF16),
            pltpu.VMEM((NH, NZ, KR, 2 * C), F32),
            pltpu.VMEM((NH, NZ, KR, 2 * C), F32),
            pltpu.VMEM((CHUNKS, NH, NZ, KR, 2 * C), BF16),
            pltpu.VMEM((CHUNKS, NH, NZ, KR, 2 * C), BF16),
            pltpu.VMEM((8, 2, 2, C, C), BF16),
            pltpu.VMEM((2, 2 * C, 2 * C), BF16),
            pltpu.VMEM((6, C, 2 * C), BF16),
            pltpu.VMEM((8, 2 * C, 2 * C), BF16),
            pltpu.VMEM((8, 2 * C, 2 * C), BF16),
            pltpu.VMEM((4, 2 * C, 2 * C), BF16),
            pltpu.VMEM((2, AMP, C), F32),
            pltpu.VMEM((NX, NZ, 2, AMP, 128), BF16),
            pltpu.VMEM((NX, NZ, 2, AMP, C), BF16),
            pltpu.VMEM((NZ, NX * AMP, 2 * C), F32),
            pltpu.VMEM((NZ, NZ, 128), F32),
            pltpu.VMEM((NX, NZ, 128), F32),
            dma((3 + CHUNKS,)),
            dma((CHUNKS,)),
            dma((CHUNKS,)),
            dma((2,)),
            dma((2,)),
            dma((2,)),
            dma((2,)),
            dma((CHUNKS,)),
            dma((CHUNKS,)),
            dma((3,)),
            dma((3,)),
        ],
        compiler_params=pltpu.CompilerParams(
            collective_id=0, has_side_effects=True, vmem_limit_bytes=56 * 1024 * 1024
        ),
        name="network",
    )(
        tensors.reshape(2, GROUP, CHUNKS, KR, C),
        gates,
        closing_rows,
        closing_columns,
    )
    out = out.reshape(2, 2, 2, NZ, 2, NX, AMP).transpose(4, 2, 3, 5, 0, 1, 6)
    return out.reshape(2, -1)


def solution(mesh):
    placed = (
        P(None, "sx", "sy", None, None),
        P(),
        P(None, ("sx", "sy"), None),
        P(None, ("sx", "sy"), None),
    )
    return jax.shard_map(local, mesh=mesh, in_specs=placed, out_specs=P(), check_vma=False)
```

```python
import functools

import jax
import jax.numpy as jnp
from jax import lax
from jax.experimental import pallas as pl
from jax.experimental.pallas import tpu as pltpu
from jax.sharding import PartitionSpec as P

MESH = pl.DeviceIdType.MESH
F32 = jnp.float32
BF16 = jnp.bfloat16
NZ, NY, NX, NC = 8, 4, 4, 2
NH = NY * NC
GROUP = NZ * NH
C = 256
CHUNKS = 4
KR = 4
UNROLL = True
AMP = 16
Z_ORDER = (4, 3, 5, 2, 6, 1, 7, 0)
Y_ORDER = (2, 1, 3, 0)


def position():
    sx = lax.axis_index("sx")
    sy = lax.axis_index("sy")
    return lax.rem(sx, 8), (sx // 8) * 2 + lax.rem(sy // 2, 2), sy // 4, lax.rem(sy, 2)


def device(z, y, x, c):
    return ((y // 2) * 8 + z, x * 4 + lax.rem(y, 2) * 2 + c)


def bits_index(y, c):
    return y // 2 + 2 * c + 4 * lax.rem(y, 2)


def ones(number):
    return bin(number).count("1")


def turned(block, power):
    power %= 4
    re, im = block[:, :C], block[:, C:]
    if power == 0:
        return block
    if power == 1:
        return jnp.concatenate([-im, re], axis=1)
    if power == 2:
        return -block
    return jnp.concatenate([im, -re], axis=1)


def hadamard(blocks):
    blocks = list(blocks)
    half = 1
    while half < len(blocks):
        for low in range(len(blocks)):
            if not low & half:
                a, b = blocks[low], blocks[low | half]
                blocks[low], blocks[low | half] = a + b, a - b
        half *= 2
    return blocks


def fill_full(full, index, re, im):
    full[index, :C, :C] = re
    full[index, :C, C:] = im
    full[index, C:, :C] = -im
    full[index, C:, C:] = re


def section_pairs(gates, first, right, tops):
    for which in range(2):
        tops[which, :, :C] = gates[first, which, 0]
        tops[which, :, C:] = gates[first, which, 1]
        fill_full(right, which, gates[first + 1, which, 0], gates[first + 1, which, 1])
    aa = jnp.dot(tops[0], right[0], preferred_element_type=F32)
    bb = jnp.dot(tops[1], right[1], preferred_element_type=F32)
    even, odd = aa - bb, aa + bb
    ba = jnp.dot(tops[1], right[0], preferred_element_type=F32)
    ab = jnp.dot(tops[0], right[1], preferred_element_type=F32)
    plus, minus = turned(ba + ab, -1), turned(ba - ab, -1)
    return even + plus, odd - minus, odd + minus, even - plus


def triple_products(gates, first, right, tops, full):
    for low, pair in enumerate(section_pairs(gates, first, right, tops)):
        tops[2 + low] = pair.astype(BF16)
    for which in range(2):
        fill_full(right, which, gates[first + 2, which, 0], gates[first + 2, which, 1])
    for low in range(4):
        with_a = jnp.dot(tops[2 + low], right[0], preferred_element_type=F32)
        with_b = turned(jnp.dot(tops[2 + low], right[1], preferred_element_type=F32), -1)
        for third, out in enumerate((with_a + with_b, with_a - with_b)):
            out = out.astype(BF16)
            full[low + 4 * third] = out


def pair_products(gates, first, right, tops, full):
    for low, pair in enumerate(section_pairs(gates, first, right, tops)):
        pair = pair.astype(BF16)
        fill_full(full, low, pair[:, :C], pair[:, C:])


def wait_bytes(ref, sem):
    pltpu.make_async_copy(ref, ref, sem).wait()


def half_turn(block):
    return pltpu.roll(block, KR, 0)


def times_gate(blocks, gate):
    left = jnp.concatenate(blocks, axis=0).astype(BF16)
    out = jnp.dot(left, gate, preferred_element_type=F32)
    sign = jnp.where(lax.broadcasted_iota(jnp.int32, (2 * KR, C), 0) < KR, -1.0, 1.0)
    result = []
    for n in range(len(blocks)):
        rows = out[n * 2 * KR : (n + 1) * 2 * KR]
        result.append(rows[:, :C] + sign * half_turn(rows[:, C:]))
    return result


def sections(q, recv, work1, work2, g_low, g_high, ret_send):
    def forward_z(h, carry):
        blocks = hadamard([recv[q, h * NZ + z].astype(F32) for z in range(NZ)])
        for t in range(NZ):
            work1[h, t] = blocks[t]
        return carry

    def forward_h(t, carry):
        blocks = times_gate(hadamard([work1[h, t] for h in range(NH)]), g_low[t])
        for h in range(NH):
            work2[h, t] = blocks[h]
        return carry

    def inverse_z(h, carry):
        blocks = hadamard(times_gate([work2[h, t] for t in range(NZ)], g_high[h]))
        for z in range(NZ):
            work1[h, z] = blocks[z]
        return carry

    def inverse_h(z, carry):
        blocks = hadamard([work1[t, z] for t in range(NH)])
        for h in range(NH):
            ret_send[q, h, z] = (blocks[h] * (1.0 / GROUP)).astype(BF16)
        return carry

    lax.fori_loop(0, NH, forward_z, 0, unroll=UNROLL)
    lax.fori_loop(0, NZ, forward_h, 0, unroll=UNROLL)
    lax.fori_loop(0, NH, inverse_z, 0, unroll=UNROLL)
    lax.fori_loop(0, NZ, inverse_h, 0, unroll=UNROLL)


def unit(turn):
    turn = lax.rem(turn, 4)
    odd = lax.rem(turn, 2)
    return ((1 - odd) * (1 - turn)).astype(F32), (odd * (2 - turn)).astype(F32)


def assemble(gathered, out_ref):
    lane = lax.broadcasted_iota(jnp.int32, (NZ, 128), 1) // AMP
    for part in range(2):
        for y_hi in range(2):
            for x_hi in range(2):
                total = None
                for x_lo in range(2):
                    for y_lo in range(2):
                        for core in range(2):
                            source = part * 4 + x_hi * 2 + x_lo
                            target = x_lo * 4 + y_lo * 2 + core
                            rows = gathered[y_hi + 2 * core + 4 * y_lo]
                            shift = (target - source) * AMP % 128
                            moved = pltpu.roll(rows, shift, 1) if shift else rows
                            total = moved if total is None else jnp.where(lane == target, moved, total)
                for z in range(NZ):
                    group = (y_hi * NZ + z) * 2 + x_hi
                    out_ref[part : part + 1, group * 128 : (group + 1) * 128] = total[z : z + 1]


def kernel(
    x_ref, gates_ref, rows_ref, cols_ref, out_ref,
    x_in, staged, recv, work1, work2, ret_send, ret, gates, right, tops, g_low, g_high, g_x,
    cols, crx, ccx, left, wbuf, finz, finx, finh,
    local_sem, main_send, main_recv, small_send, small_recv, x_send, x_recv, back_send, back_recv, fin_send, fin_recv,
):
    mz, my, mx, mc = position()
    mh = bits_index(my, mc)
    mine = mh * NZ + mz
    z0, z1, z2 = lax.rem(mz, 2), lax.rem(mz // 2, 2), mz // 4
    h_ones = my // 2 + lax.rem(my, 2) + mc

    z_peers = [lax.rem(mz + d, NZ) for d in range(NZ)]
    y_peers = [lax.rem(my + d, NY) for d in range(NY)]
    c_peers = [lax.rem(mc + d, NC) for d in range(NC)]
    x_peers = [lax.rem(mx + d, NX) for d in range(NX)]
    group = [(dz, dy, dc) for dz in Z_ORDER for dy in Y_ORDER for dc in range(NC) if dz or dy or dc]
    back = [(dy, dc) for dy in Y_ORDER for dc in range(NC) if dy or dc]

    x_copy = pltpu.make_async_copy(x_ref, x_in, local_sem.at[3])
    x_copy.start()
    cols_copy = pltpu.make_async_copy(cols_ref, cols, local_sem.at[1])
    cols_copy.start()
    own_rows = pltpu.make_async_copy(rows_ref.at[:, :, pl.ds(pl.multiple_of(mz * 128, 128), 128)], crx.at[mx, mz], local_sem.at[2])
    own_rows.start()
    gates_copy = pltpu.make_async_copy(gates_ref, gates, local_sem.at[0])
    gates_copy.start()

    barrier = pltpu.get_barrier_semaphore()
    for dz, dy, dc in group:
        pl.semaphore_signal(barrier, inc=1, device_id=device(z_peers[dz], y_peers[dy], mx, c_peers[dc]), device_id_type=MESH)
    for dx in range(1, NX):
        pl.semaphore_signal(barrier, inc=1, device_id=device(mz, my, x_peers[dx], mc), device_id_type=MESH)

    cos, sin = unit(z0 + z1 + z2 + h_ones)
    low = lax.broadcasted_iota(jnp.int32, (2 * KR, C), 0) < KR

    def stage(target, carry):
        re = x_in[0, target].astype(F32)
        im = x_in[1, target].astype(F32)
        re, im = cos * re - sin * im, cos * im + sin * re
        for half in range(2):
            a, b = re[8 * half : 8 * half + 8], im[8 * half : 8 * half + 8]
            staged[2 * half, target] = jnp.where(low, a, half_turn(b)).astype(BF16)
            staged[2 * half + 1, target] = jnp.where(low, half_turn(a), b).astype(BF16)
        return carry

    cols_copy.wait()
    ccx[mx, mz] = cols[...].astype(BF16)
    x_copy.wait()
    lax.fori_loop(0, GROUP, stage, 0, unroll=4)
    for q in range(CHUNKS):
        recv[q, mine] = staged[q, mz * NH + mh]
    pl.semaphore_wait(barrier, GROUP - 1 + NX - 1)

    def remote(src, dst, send, recv_sem, where):
        copy = pltpu.make_async_remote_copy(
            src_ref=src, dst_ref=dst, send_sem=send, recv_sem=recv_sem, device_id=device(*where), device_id_type=MESH
        )
        copy.start()

    for dz in Z_ORDER[:-1]:
        pz = z_peers[dz]
        there = (pz, my, mx, mc)
        columns = pl.ds(pl.multiple_of(pz * 128, 128), 128)
        remote(rows_ref.at[:, :, columns], crx.at[mx, mz], small_send.at[0], small_recv.at[0], there)
        remote(ccx.at[mx, mz], ccx.at[mx, mz], small_send.at[1], small_recv.at[1], there)
    for q in range(CHUNKS):
        for dz, dy, dc in group:
            pz, py, pc = z_peers[dz], y_peers[dy], c_peers[dc]
            block = pz * NH + bits_index(py, pc)
            remote(staged.at[q, block], recv.at[q, mine], main_send.at[q], main_recv.at[q], (pz, py, mx, pc))

    gates_copy.wait()
    triple_products(gates, 0, right, tops, g_low)
    triple_products(gates, 3, right, tops, g_high)
    pair_products(gates, 6, right, tops, g_x)

    own_rows.wait()
    wait_bytes(crx.at[0, pl.ds(0, NZ - 1)], small_recv.at[0])
    wait_bytes(ccx.at[0, pl.ds(0, NZ - 1)], small_recv.at[1])
    for dx in (2, 1, 3):
        there = (mz, my, x_peers[dx], mc)
        remote(crx.at[mx], crx.at[mx], x_send.at[0], x_recv.at[0], there)
        remote(ccx.at[mx], ccx.at[mx], x_send.at[1], x_recv.at[1], there)

    def closing_rows_in_order():
        row = lax.broadcasted_iota(jnp.int32, (128, 2 * C), 0)
        column = lax.broadcasted_iota(jnp.int32, (128, 2 * C), 1)
        wanted = (row // KR) * 2 * KR + lax.rem(row, KR)
        wanted = jnp.where(column < C, wanted, wanted + C + KR)
        select = jnp.where(column == wanted, 1.0, 0.0).astype(BF16)
        for z in range(NZ):
            rows = [crx[xs, z, part] for part in range(2) for xs in range(NX)]
            out = jnp.dot(jnp.concatenate(rows, axis=0), select, preferred_element_type=F32)
            half = NX * AMP
            for_re = out[:half, :C] - out[half:, C:]
            for_im = out[half:, :C] + out[:half, C:]
            left[z] = jnp.concatenate([for_re, for_im], axis=0).astype(BF16)

    def columns_through_x():
        m0, m1 = lax.rem(mx, 2), mx // 2
        for xs in range(NX):
            parts = []
            for z in range(NZ):
                both = ccx[xs, z]
                parts.append(jnp.concatenate([both[0], -both[1]], axis=1))
            vectors = jnp.concatenate(parts, axis=0)
            s0, s1 = xs % 2, xs // 2
            e0 = s0 + m0 - 2 * s0 * m0
            e1 = s1 + m1 - 2 * s1 * m1
            f0 = (1 - 2 * e0).astype(F32)
            f1 = (1 - 2 * e1).astype(F32)
            cos, sin = unit(m0 + m1 - s0 - s1 - h_ones + 8)
            total = None
            for t in range(4):
                u = lax.dot_general(vectors, g_x[t], (((1,), (1,)), ((), ())), preferred_element_type=F32)
                if t & 1:
                    u = u * f0
                if t & 2:
                    u = u * f1
                total = u if total is None else total + u
            total = total * 0.25
            re, neg = total[:, :C], total[:, C:]
            re, neg = cos * re + sin * neg, cos * neg - sin * re
            for z in range(NZ):
                a, b = re[z * AMP : (z + 1) * AMP], neg[z * AMP : (z + 1) * AMP]
                a, b = ((a, b), (-b, a), (-a, -b), (b, -a))[ones(z)]
                wbuf[z, xs * AMP : (xs + 1) * AMP, :C] = a
                wbuf[z, xs * AMP : (xs + 1) * AMP, C:] = b

    for q in range(CHUNKS):
        wait_bytes(recv.at[q, pl.ds(0, GROUP - 1)], main_recv.at[q])
        sections(q, recv, work1, work2, g_low, g_high, ret_send)
        for dy, dc in back:
            py, pc = y_peers[dy], c_peers[dc]
            remote(ret_send.at[q, bits_index(py, pc)], ret.at[q, mh], back_send.at[q], back_recv.at[q], (mz, py, mx, pc))
        ret[q, mh] = ret_send[q, mh]
        if q == 0:
            wait_bytes(crx.at[pl.ds(0, NX - 1)], x_recv.at[0])
            wait_bytes(ccx.at[pl.ds(0, NX - 1)], x_recv.at[1])
            closing_rows_in_order()
            columns_through_x()

    for q in range(CHUNKS):
        wait_bytes(ret.at[q, pl.ds(0, NH - 1)], back_recv.at[q])

    def close(z, carry):
        blocks = []
        for h in range(NH):
            for q in range(CHUNKS):
                blocks.append(ret[q, h, z].astype(F32))
        tensor = jnp.concatenate(blocks, axis=0).astype(BF16)
        proj = jnp.dot(left[z], tensor, preferred_element_type=F32)
        half = NX * AMP
        p_re, p_im = proj[:half], proj[half:]
        w = wbuf[z]
        w_re, w_neg = w[:, :C], w[:, C:]
        a_re = p_re * w_re + p_im * w_neg
        a_im = p_im * w_re - p_re * w_neg
        both = jnp.concatenate([a_re[:, :128] + a_re[:, 128:], a_im[:, :128] + a_im[:, 128:]], axis=0)
        finz[mz, pl.ds(z, 1)] = jnp.sum(jnp.transpose(both), axis=0, keepdims=True)
        return carry

    lax.fori_loop(0, NZ, close, 0, unroll=UNROLL)

    for dz in Z_ORDER[:-1]:
        remote(finz.at[mz], finz.at[mz], fin_send.at[0], fin_recv.at[0], (z_peers[dz], my, mx, mc))
    wait_bytes(crx.at[0, pl.ds(0, NZ - 1)], small_send.at[0])
    wait_bytes(ccx.at[0, pl.ds(0, NZ - 1)], small_send.at[1])
    wait_bytes(crx.at[pl.ds(0, NX - 1)], x_send.at[0])
    wait_bytes(ccx.at[pl.ds(0, NX - 1)], x_send.at[1])
    for q in range(CHUNKS):
        wait_bytes(recv.at[q, pl.ds(0, GROUP - 1)], main_send.at[q])
        wait_bytes(ret.at[q, pl.ds(0, NH - 1)], back_send.at[q])
    wait_bytes(finz.at[pl.ds(0, NZ - 1)], fin_recv.at[0])
    finx[mx] = jnp.sum(finz[...], axis=0)
    for dx in (2, 1, 3):
        remote(finx.at[mx], finx.at[mx], fin_send.at[1], fin_recv.at[1], (mz, my, x_peers[dx], mc))
    wait_bytes(finz.at[pl.ds(0, NZ - 1)], fin_send.at[0])
    wait_bytes(finx.at[pl.ds(0, NX - 1)], fin_recv.at[1])
    finh[mh] = jnp.sum(finx[...], axis=0)
    for dy, dc in back:
        remote(finh.at[mh], finh.at[mh], fin_send.at[2], fin_recv.at[2], (mz, y_peers[dy], mx, c_peers[dc]))
    wait_bytes(finx.at[pl.ds(0, NX - 1)], fin_send.at[1])
    wait_bytes(finh.at[pl.ds(0, NH - 1)], fin_recv.at[2])
    assemble(finh, out_ref)
    wait_bytes(finh.at[pl.ds(0, NH - 1)], fin_send.at[2])


def local(tensors, gates, closing_rows, closing_columns):
    dma = pltpu.SemaphoreType.DMA
    return pl.pallas_call(
        kernel,
        out_shape=jax.ShapeDtypeStruct((2, NZ * NH * NX * AMP), F32),
        in_specs=[pl.BlockSpec(memory_space=pl.ANY)] * 4,
        out_specs=pl.BlockSpec(memory_space=pltpu.VMEM),
        scratch_shapes=[
            pltpu.VMEM((2, GROUP, 16, C), BF16),
            pltpu.VMEM((CHUNKS, GROUP, 2 * KR, C), BF16),
            pltpu.VMEM((CHUNKS, GROUP, 2 * KR, C), BF16),
            pltpu.VMEM((NH, NZ, 2 * KR, C), F32),
            pltpu.VMEM((NH, NZ, 2 * KR, C), F32),
            pltpu.VMEM((CHUNKS, NH, NZ, 2 * KR, C), BF16),
            pltpu.VMEM((CHUNKS, NH, NZ, 2 * KR, C), BF16),
            pltpu.VMEM((8, 2, 2, C, C), BF16),
            pltpu.VMEM((2, 2 * C, 2 * C), BF16),
            pltpu.VMEM((6, C, 2 * C), BF16),
            pltpu.VMEM((8, C, 2 * C), BF16),
            pltpu.VMEM((8, C, 2 * C), BF16),
            pltpu.VMEM((4, 2 * C, 2 * C), BF16),
            pltpu.VMEM((2, AMP, C), F32),
            pltpu.VMEM((NX, NZ, 2, AMP, 128), BF16),
            pltpu.VMEM((NX, NZ, 2, AMP, C), BF16),
            pltpu.VMEM((NZ, 128, C), BF16),
            pltpu.VMEM((NZ, NX * AMP, 2 * C), F32),
            pltpu.VMEM((NZ, NZ, 128), F32),
            pltpu.VMEM((NX, NZ, 128), F32),
            pltpu.VMEM((NH, NZ, 128), F32),
            dma((4,)),
            dma((CHUNKS,)),
            dma((CHUNKS,)),
            dma((2,)),
            dma((2,)),
            dma((2,)),
            dma((2,)),
            dma((CHUNKS,)),
            dma((CHUNKS,)),
            dma((3,)),
            dma((3,)),
        ],
        compiler_params=pltpu.CompilerParams(
            collective_id=0, has_side_effects=True, vmem_limit_bytes=56 * 1024 * 1024
        ),
        name="network",
    )(tensors.reshape(2, GROUP, 16, C), gates, closing_rows, closing_columns)


def solution(mesh):
    placed = (
        P(None, "sx", "sy", None, None),
        P(),
        P(None, ("sx", "sy"), None),
        P(None, ("sx", "sy"), None),
    )
    return jax.shard_map(local, mesh=mesh, in_specs=placed, out_specs=P(), check_vma=False)
```

```python
import functools

import jax
import jax.numpy as jnp
from jax import lax
from jax.experimental import pallas as pl
from jax.experimental.pallas import tpu as pltpu
from jax.sharding import PartitionSpec as P

MESH = pl.DeviceIdType.MESH
F32 = jnp.float32
BF16 = jnp.bfloat16
NZ, NY, NX, NC = 8, 4, 4, 2
NH = NY * NC
GROUP = NZ * NH
C = 256
CHUNKS = 4
KR = 4
UNROLL = True
AMP = 16
Z_ORDER = (4, 3, 5, 2, 6, 1, 7, 0)
Y_ORDER = (2, 1, 3, 0)


def position():
    sx = lax.axis_index("sx")
    sy = lax.axis_index("sy")
    return lax.rem(sx, 8), (sx // 8) * 2 + lax.rem(sy // 2, 2), sy // 4, lax.rem(sy, 2)


def device(z, y, x, c):
    return ((y // 2) * 8 + z, x * 4 + lax.rem(y, 2) * 2 + c)


def bits_index(y, c):
    return y // 2 + 2 * c + 4 * lax.rem(y, 2)


def ones(number):
    return bin(number).count("1")


def turned(block, power):
    power %= 4
    re, im = block[:, :C], block[:, C:]
    if power == 0:
        return block
    if power == 1:
        return jnp.concatenate([-im, re], axis=1)
    if power == 2:
        return -block
    return jnp.concatenate([im, -re], axis=1)


def hadamard(blocks):
    blocks = list(blocks)
    half = 1
    while half < len(blocks):
        for low in range(len(blocks)):
            if not low & half:
                a, b = blocks[low], blocks[low | half]
                blocks[low], blocks[low | half] = a + b, a - b
        half *= 2
    return blocks


def fill_full(full, index, re, im):
    full[index, :C, :C] = re
    full[index, :C, C:] = im
    full[index, C:, :C] = -im
    full[index, C:, C:] = re


def section_pairs(gates, first, right, tops):
    for which in range(2):
        tops[which, :, :C] = gates[first, which, 0]
        tops[which, :, C:] = gates[first, which, 1]
        fill_full(right, which, gates[first + 1, which, 0], gates[first + 1, which, 1])
    aa = jnp.dot(tops[0], right[0], preferred_element_type=F32)
    bb = jnp.dot(tops[1], right[1], preferred_element_type=F32)
    even, odd = aa - bb, aa + bb
    ba = jnp.dot(tops[1], right[0], preferred_element_type=F32)
    ab = jnp.dot(tops[0], right[1], preferred_element_type=F32)
    plus, minus = turned(ba + ab, -1), turned(ba - ab, -1)
    return even + plus, odd - minus, odd + minus, even - plus


def triple_products(gates, first, right, tops, full):
    for low, pair in enumerate(section_pairs(gates, first, right, tops)):
        tops[2 + low] = pair.astype(BF16)
    for which in range(2):
        fill_full(right, which, gates[first + 2, which, 0], gates[first + 2, which, 1])
    for low in range(4):
        with_a = jnp.dot(tops[2 + low], right[0], preferred_element_type=F32)
        with_b = turned(jnp.dot(tops[2 + low], right[1], preferred_element_type=F32), -1)
        for third, out in enumerate((with_a + with_b, with_a - with_b)):
            out = out.astype(BF16)
            full[low + 4 * third] = out


def pair_products(gates, first, right, tops, full):
    for low, pair in enumerate(section_pairs(gates, first, right, tops)):
        pair = pair.astype(BF16)
        fill_full(full, low, pair[:, :C], pair[:, C:])


def wait_bytes(ref, sem):
    pltpu.make_async_copy(ref, ref, sem).wait()


def half_turn(block):
    return pltpu.roll(block, KR, 0)


def times_gate(blocks, gate):
    left = jnp.concatenate(blocks, axis=0).astype(BF16)
    out = jnp.dot(left, gate, preferred_element_type=F32)
    sign = jnp.where(lax.broadcasted_iota(jnp.int32, (2 * KR, C), 0) < KR, -1.0, 1.0)
    result = []
    for n in range(len(blocks)):
        rows = out[n * 2 * KR : (n + 1) * 2 * KR]
        result.append(rows[:, :C] + sign * half_turn(rows[:, C:]))
    return result


def sections(q, recv, work1, work2, g_low, g_high, ret_send):
    def forward_z(h, carry):
        blocks = hadamard([recv[q, h * NZ + z].astype(F32) for z in range(NZ)])
        for t in range(NZ):
            work1[h, t] = blocks[t]
        return carry

    def forward_h(t, carry):
        blocks = times_gate(hadamard([work1[h, t] for h in range(NH)]), g_low[t])
        for h in range(NH):
            work2[h, t] = blocks[h]
        return carry

    def inverse_z(h, carry):
        blocks = hadamard(times_gate([work2[h, t] for t in range(NZ)], g_high[h]))
        for z in range(NZ):
            work1[h, z] = blocks[z]
        return carry

    def inverse_h(z, carry):
        blocks = hadamard([work1[t, z] for t in range(NH)])
        for h in range(NH):
            ret_send[q, h, z] = (blocks[h] * (1.0 / GROUP)).astype(BF16)
        return carry

    lax.fori_loop(0, NH, forward_z, 0, unroll=UNROLL)
    lax.fori_loop(0, NZ, forward_h, 0, unroll=UNROLL)
    lax.fori_loop(0, NH, inverse_z, 0, unroll=UNROLL)
    lax.fori_loop(0, NZ, inverse_h, 0, unroll=UNROLL)


def unit(turn):
    turn = lax.rem(turn, 4)
    odd = lax.rem(turn, 2)
    return ((1 - odd) * (1 - turn)).astype(F32), (odd * (2 - turn)).astype(F32)


def assemble(gathered, out_ref):
    lane = lax.broadcasted_iota(jnp.int32, (NZ, 128), 1) // AMP
    for part in range(2):
        for y_hi in range(2):
            for x_hi in range(2):
                total = None
                for x_lo in range(2):
                    for y_lo in range(2):
                        for core in range(2):
                            source = part * 4 + x_hi * 2 + x_lo
                            target = x_lo * 4 + y_lo * 2 + core
                            rows = gathered[y_hi + 2 * core + 4 * y_lo]
                            shift = (target - source) * AMP % 128
                            moved = pltpu.roll(rows, shift, 1) if shift else rows
                            total = moved if total is None else jnp.where(lane == target, moved, total)
                for z in range(NZ):
                    group = (y_hi * NZ + z) * 2 + x_hi
                    out_ref[part : part + 1, group * 128 : (group + 1) * 128] = total[z : z + 1]


def kernel(
    x_ref, gates_ref, rows_ref, cols_ref, out_ref,
    x_in, staged, recv, work1, work2, ret_send, ret, gates, right, tops, g_low, g_high, g_x,
    cols, crx, ccx, left, wbuf, finz, finx, finh,
    local_sem, main_send, main_recv, small_send, small_recv, x_send, x_recv, back_send, back_recv, fin_send, fin_recv, ready,
):
    mz, my, mx, mc = position()
    mh = bits_index(my, mc)
    mine = mh * NZ + mz
    z0, z1, z2 = lax.rem(mz, 2), lax.rem(mz // 2, 2), mz // 4
    h_ones = my // 2 + lax.rem(my, 2) + mc

    z_peers = [lax.rem(mz + d, NZ) for d in range(NZ)]
    y_peers = [lax.rem(my + d, NY) for d in range(NY)]
    c_peers = [lax.rem(mc + d, NC) for d in range(NC)]
    x_peers = [lax.rem(mx + d, NX) for d in range(NX)]
    back = [(dy, dc) for dy in Y_ORDER for dc in range(NC) if dy or dc]

    x_copy = pltpu.make_async_copy(x_ref, x_in, local_sem.at[3])
    x_copy.start()
    cols_copy = pltpu.make_async_copy(cols_ref, cols, local_sem.at[1])
    cols_copy.start()
    own_rows = pltpu.make_async_copy(rows_ref.at[:, :, pl.ds(pl.multiple_of(mz * 128, 128), 128)], crx.at[mx, mz], local_sem.at[2])
    own_rows.start()
    gates_copy = pltpu.make_async_copy(gates_ref, gates, local_sem.at[0])
    gates_copy.start()

    barrier = pltpu.get_barrier_semaphore()
    near = [(mz, y_peers[dy], mx, c_peers[dc]) for dy, dc in back]
    near += [(z_peers[dz], my, mx, mc) for dz in (1, NZ - 1)]
    near += [(mz, my, x_peers[dx], mc) for dx in range(1, NX)]
    for there in near:
        pl.semaphore_signal(barrier, inc=1, device_id=device(*there), device_id_type=MESH)

    cos, sin = unit(z0 + z1 + z2 + h_ones)
    low = lax.broadcasted_iota(jnp.int32, (2 * KR, C), 0) < KR

    def stage(target, carry):
        re = x_in[0, target].astype(F32)
        im = x_in[1, target].astype(F32)
        re, im = cos * re - sin * im, cos * im + sin * re
        for half in range(2):
            a, b = re[8 * half : 8 * half + 8], im[8 * half : 8 * half + 8]
            staged[2 * half, target] = jnp.where(low, a, half_turn(b)).astype(BF16)
            staged[2 * half + 1, target] = jnp.where(low, half_turn(a), b).astype(BF16)
        return carry

    cols_copy.wait()
    ccx[mx, mz] = cols[...].astype(BF16)
    x_copy.wait()
    lax.fori_loop(0, GROUP, stage, 0, unroll=4)
    for q in range(CHUNKS):
        recv[q, mine] = staged[q, mz * NH + mh]
    pl.semaphore_wait(barrier, len(near))

    def remote(src, dst, send, recv_sem, where):
        copy = pltpu.make_async_remote_copy(
            src_ref=src, dst_ref=dst, send_sem=send, recv_sem=recv_sem, device_id=device(*where), device_id_type=MESH
        )
        copy.start()

    def send_rows(dz):
        pz = z_peers[dz]
        columns = pl.ds(pl.multiple_of(pz * 128, 128), 128)
        remote(rows_ref.at[:, :, columns], crx.at[mx, mz], small_send.at[0], small_recv.at[0], (pz, my, mx, mc))

    def send_columns(origin, dz, which):
        slot = ccx.at[mx, z_peers[origin]]
        remote(slot, slot, small_send.at[which], small_recv.at[which], (z_peers[dz], my, mx, mc))

    def send_tensor(q, dz):
        for dy in Y_ORDER:
            for dc in range(NC):
                if dz or dy or dc:
                    pz, py, pc = z_peers[dz], y_peers[dy], c_peers[dc]
                    block = pz * NH + bits_index(py, pc)
                    remote(staged.at[q, block], recv.at[q, mine], main_send.at[q], main_recv.at[q], (pz, py, mx, pc))

    send_tensor(0, 0)
    for level in range(4):
        pl.semaphore_signal(ready.at[level, 0], inc=1, device_id=device(z_peers[1], my, mx, mc), device_id_type=MESH)
        pl.semaphore_signal(ready.at[level, 1], inc=1, device_id=device(z_peers[7], my, mx, mc), device_id_type=MESH)
        distances = (level + 1, NZ - level - 1) if level < 3 else (4,)
        for dz in distances:
            send_rows(dz)
            send_columns(0, dz, 1)
        pl.semaphore_wait(ready.at[level, 0], 1)
        pl.semaphore_wait(ready.at[level, 1], 1)
        for dz in distances:
            send_tensor(0, dz)
    for dz in Z_ORDER:
        send_tensor(1, dz)

    for q in range(2, CHUNKS):
        for dz in Z_ORDER:
            send_tensor(q, dz)

    gates_copy.wait()
    triple_products(gates, 0, right, tops, g_low)
    triple_products(gates, 3, right, tops, g_high)
    pair_products(gates, 6, right, tops, g_x)

    own_rows.wait()
    wait_bytes(crx.at[0, pl.ds(0, NZ - 1)], small_recv.at[0])
    wait_bytes(ccx.at[0, pl.ds(0, 7)], small_recv.at[1])
    for dx in (2, 1, 3):
        there = (mz, my, x_peers[dx], mc)
        remote(crx.at[mx], crx.at[mx], x_send.at[0], x_recv.at[0], there)
        remote(ccx.at[mx], ccx.at[mx], x_send.at[1], x_recv.at[1], there)

    def closing_rows_in_order():
        row = lax.broadcasted_iota(jnp.int32, (128, 2 * C), 0)
        column = lax.broadcasted_iota(jnp.int32, (128, 2 * C), 1)
        wanted = (row // KR) * 2 * KR + lax.rem(row, KR)
        wanted = jnp.where(column < C, wanted, wanted + C + KR)
        select = jnp.where(column == wanted, 1.0, 0.0).astype(BF16)
        for z in range(NZ):
            rows = [crx[xs, z, part] for part in range(2) for xs in range(NX)]
            out = jnp.dot(jnp.concatenate(rows, axis=0), select, preferred_element_type=F32)
            half = NX * AMP
            for_re = out[:half, :C] - out[half:, C:]
            for_im = out[half:, :C] + out[:half, C:]
            left[z] = jnp.concatenate([for_re, for_im], axis=0).astype(BF16)

    def columns_through_x():
        m0, m1 = lax.rem(mx, 2), mx // 2
        for xs in range(NX):
            parts = []
            for z in range(NZ):
                both = ccx[xs, z]
                parts.append(jnp.concatenate([both[0], -both[1]], axis=1))
            vectors = jnp.concatenate(parts, axis=0)
            s0, s1 = xs % 2, xs // 2
            e0 = s0 + m0 - 2 * s0 * m0
            e1 = s1 + m1 - 2 * s1 * m1
            f0 = (1 - 2 * e0).astype(F32)
            f1 = (1 - 2 * e1).astype(F32)
            cos, sin = unit(m0 + m1 - s0 - s1 - h_ones + 8)
            total = None
            for t in range(4):
                u = lax.dot_general(vectors, g_x[t], (((1,), (1,)), ((), ())), preferred_element_type=F32)
                if t & 1:
                    u = u * f0
                if t & 2:
                    u = u * f1
                total = u if total is None else total + u
            re, neg = total[:, :C], total[:, C:]
            re, neg = cos * re + sin * neg, cos * neg - sin * re
            for z in range(NZ):
                a, b = re[z * AMP : (z + 1) * AMP], neg[z * AMP : (z + 1) * AMP]
                a, b = ((a, b), (-b, a), (-a, -b), (b, -a))[ones(z)]
                wbuf[z, xs * AMP : (xs + 1) * AMP, :C] = a
                wbuf[z, xs * AMP : (xs + 1) * AMP, C:] = b

    for q in range(CHUNKS):
        wait_bytes(recv.at[q, pl.ds(0, GROUP - 1)], main_recv.at[q])
        sections(q, recv, work1, work2, g_low, g_high, ret_send)
        for dy, dc in back:
            py, pc = y_peers[dy], c_peers[dc]
            remote(ret_send.at[q, bits_index(py, pc)], ret.at[q, mh], back_send.at[q], back_recv.at[q], (mz, py, mx, pc))
        ret[q, mh] = ret_send[q, mh]
        if q == 0:
            wait_bytes(crx.at[pl.ds(0, NX - 1)], x_recv.at[0])
            wait_bytes(ccx.at[pl.ds(0, NX - 1)], x_recv.at[1])
            closing_rows_in_order()
            columns_through_x()

    for q in range(CHUNKS):
        wait_bytes(ret.at[q, pl.ds(0, NH - 1)], back_recv.at[q])

    def close(z, carry):
        blocks = []
        for h in range(NH):
            for q in range(CHUNKS):
                blocks.append(ret[q, h, z].astype(F32))
        tensor = jnp.concatenate(blocks, axis=0).astype(BF16)
        proj = jnp.dot(left[z], tensor, preferred_element_type=F32)
        half = NX * AMP
        p_re, p_im = proj[:half], proj[half:]
        w = wbuf[z]
        w_re, w_neg = w[:, :C], w[:, C:]
        a_re = p_re * w_re + p_im * w_neg
        a_im = p_im * w_re - p_re * w_neg
        both = jnp.concatenate([a_re[:, :128] + a_re[:, 128:], a_im[:, :128] + a_im[:, 128:]], axis=0)
        finz[mz, pl.ds(z, 1)] = jnp.sum(jnp.transpose(both), axis=0, keepdims=True)
        return carry

    lax.fori_loop(0, NZ, close, 0, unroll=UNROLL)

    for dz in Z_ORDER[:-1]:
        remote(finz.at[mz], finz.at[mz], fin_send.at[0], fin_recv.at[0], (z_peers[dz], my, mx, mc))
    wait_bytes(crx.at[0, pl.ds(0, NZ - 1)], small_send.at[0])
    wait_bytes(ccx.at[0, pl.ds(0, 7)], small_send.at[1])
    wait_bytes(crx.at[pl.ds(0, NX - 1)], x_send.at[0])
    wait_bytes(ccx.at[pl.ds(0, NX - 1)], x_send.at[1])
    for q in range(CHUNKS):
        wait_bytes(recv.at[q, pl.ds(0, GROUP - 1)], main_send.at[q])
        wait_bytes(ret.at[q, pl.ds(0, NH - 1)], back_send.at[q])
    wait_bytes(finz.at[pl.ds(0, NZ - 1)], fin_recv.at[0])
    finx[mx] = jnp.sum(finz[...], axis=0)
    for dx in (2, 1, 3):
        remote(finx.at[mx], finx.at[mx], fin_send.at[1], fin_recv.at[1], (mz, my, x_peers[dx], mc))
    wait_bytes(finz.at[pl.ds(0, NZ - 1)], fin_send.at[0])
    wait_bytes(finx.at[pl.ds(0, NX - 1)], fin_recv.at[1])
    finh[mh] = jnp.sum(finx[...], axis=0)
    for dy, dc in back:
        remote(finh.at[mh], finh.at[mh], fin_send.at[2], fin_recv.at[2], (mz, y_peers[dy], mx, c_peers[dc]))
    wait_bytes(finx.at[pl.ds(0, NX - 1)], fin_send.at[1])
    wait_bytes(finh.at[pl.ds(0, NH - 1)], fin_recv.at[2])
    assemble(finh, out_ref)
    wait_bytes(finh.at[pl.ds(0, NH - 1)], fin_send.at[2])


def local(tensors, gates, closing_rows, closing_columns):
    dma = pltpu.SemaphoreType.DMA
    out = pl.pallas_call(
        kernel,
        out_shape=jax.ShapeDtypeStruct((2, NZ * NH * NX * AMP), F32),
        in_specs=[pl.BlockSpec(memory_space=pl.ANY)] * 4,
        out_specs=pl.BlockSpec(memory_space=pltpu.VMEM),
        scratch_shapes=[
            pltpu.VMEM((2, GROUP, 16, C), BF16),
            pltpu.VMEM((CHUNKS, GROUP, 2 * KR, C), BF16),
            pltpu.VMEM((CHUNKS, GROUP, 2 * KR, C), BF16),
            pltpu.VMEM((NH, NZ, 2 * KR, C), F32),
            pltpu.VMEM((NH, NZ, 2 * KR, C), F32),
            pltpu.VMEM((CHUNKS, NH, NZ, 2 * KR, C), BF16),
            pltpu.VMEM((CHUNKS, NH, NZ, 2 * KR, C), BF16),
            pltpu.VMEM((8, 2, 2, C, C), BF16),
            pltpu.VMEM((2, 2 * C, 2 * C), BF16),
            pltpu.VMEM((6, C, 2 * C), BF16),
            pltpu.VMEM((8, C, 2 * C), BF16),
            pltpu.VMEM((8, C, 2 * C), BF16),
            pltpu.VMEM((4, 2 * C, 2 * C), BF16),
            pltpu.VMEM((2, AMP, C), F32),
            pltpu.VMEM((NX, NZ, 2, AMP, 128), BF16),
            pltpu.VMEM((NX, NZ, 2, AMP, C), BF16),
            pltpu.VMEM((NZ, 128, C), BF16),
            pltpu.VMEM((NZ, NX * AMP, 2 * C), F32),
            pltpu.VMEM((NZ, NZ, 128), F32),
            pltpu.VMEM((NX, NZ, 128), F32),
            pltpu.VMEM((NH, NZ, 128), F32),
            dma((4,)),
            dma((CHUNKS,)),
            dma((CHUNKS,)),
            dma((3,)),
            dma((3,)),
            dma((2,)),
            dma((2,)),
            dma((CHUNKS,)),
            dma((CHUNKS,)),
            dma((3,)),
            dma((3,)),
            pltpu.SemaphoreType.REGULAR((4, 2)),
        ],
        compiler_params=pltpu.CompilerParams(
            collective_id=0, has_side_effects=True, vmem_limit_bytes=56 * 1024 * 1024
        ),
        name="network",
    )(tensors.reshape(2, GROUP, 16, C), gates, closing_rows, closing_columns)
    return out * (1.0 / NX)


def solution(mesh):
    placed = (
        P(None, "sx", "sy", None, None),
        P(),
        P(None, ("sx", "sy"), None),
        P(None, ("sx", "sy"), None),
    )
    return jax.shard_map(local, mesh=mesh, in_specs=placed, out_specs=P(), check_vma=False)
```

```python
import functools

import jax
import jax.numpy as jnp
from jax import lax
from jax.experimental import pallas as pl
from jax.experimental.pallas import tpu as pltpu
from jax.sharding import PartitionSpec as P

MESH = pl.DeviceIdType.MESH
F32 = jnp.float32
BF16 = jnp.bfloat16
NZ, NY, NX, NC = 8, 4, 4, 2
NH = NY * NC
GROUP = NZ * NH
C = 256
CHUNKS = 4
KR = 4
UNROLL = True
AMP = 16
Z_ORDER = (4, 3, 5, 2, 6, 1, 7, 0)
Y_ORDER = (2, 1, 3, 0)


def position():
    sx = lax.axis_index("sx")
    sy = lax.axis_index("sy")
    return lax.rem(sx, 8), (sx // 8) * 2 + lax.rem(sy // 2, 2), sy // 4, lax.rem(sy, 2)


def device(z, y, x, c):
    return ((y // 2) * 8 + z, x * 4 + lax.rem(y, 2) * 2 + c)


def bits_index(y, c):
    return y // 2 + 2 * c + 4 * lax.rem(y, 2)


def ones(number):
    return bin(number).count("1")


def turned(block, power):
    power %= 4
    re, im = block[:, :C], block[:, C:]
    if power == 0:
        return block
    if power == 1:
        return jnp.concatenate([-im, re], axis=1)
    if power == 2:
        return -block
    return jnp.concatenate([im, -re], axis=1)


def hadamard(blocks):
    blocks = list(blocks)
    half = 1
    while half < len(blocks):
        for low in range(len(blocks)):
            if not low & half:
                a, b = blocks[low], blocks[low | half]
                blocks[low], blocks[low | half] = a + b, a - b
        half *= 2
    return blocks


def fill_full(full, index, re, im):
    full[index, :C, :C] = re
    full[index, :C, C:] = im
    full[index, C:, :C] = -im
    full[index, C:, C:] = re


def section_pairs(gates, first, right, tops):
    for which in range(2):
        tops[which, :, :C] = gates[first, which, 0]
        tops[which, :, C:] = gates[first, which, 1]
        fill_full(right, which, gates[first + 1, which, 0], gates[first + 1, which, 1])
    aa = jnp.dot(tops[0], right[0], preferred_element_type=F32)
    bb = jnp.dot(tops[1], right[1], preferred_element_type=F32)
    even, odd = aa - bb, aa + bb
    ba = jnp.dot(tops[1], right[0], preferred_element_type=F32)
    ab = jnp.dot(tops[0], right[1], preferred_element_type=F32)
    plus, minus = turned(ba + ab, -1), turned(ba - ab, -1)
    return even + plus, odd - minus, odd + minus, even - plus


def triple_products(gates, first, right, tops, full):
    for low, pair in enumerate(section_pairs(gates, first, right, tops)):
        tops[2 + low] = pair.astype(BF16)
    for which in range(2):
        fill_full(right, which, gates[first + 2, which, 0], gates[first + 2, which, 1])
    for low in range(4):
        with_a = jnp.dot(tops[2 + low], right[0], preferred_element_type=F32)
        with_b = turned(jnp.dot(tops[2 + low], right[1], preferred_element_type=F32), -1)
        for third, out in enumerate((with_a + with_b, with_a - with_b)):
            out = out.astype(BF16)
            full[low + 4 * third] = out


def pair_products(gates, first, right, tops, full):
    for low, pair in enumerate(section_pairs(gates, first, right, tops)):
        pair = pair.astype(BF16)
        fill_full(full, low, pair[:, :C], pair[:, C:])


def wait_bytes(ref, sem):
    pltpu.make_async_copy(ref, ref, sem).wait()


def half_turn(block):
    return pltpu.roll(block, KR, 0)


def times_gate(blocks, gate):
    left = jnp.concatenate(blocks, axis=0).astype(BF16)
    out = jnp.dot(left, gate, preferred_element_type=F32)
    sign = jnp.where(lax.broadcasted_iota(jnp.int32, (2 * KR, C), 0) < KR, -1.0, 1.0)
    result = []
    for n in range(len(blocks)):
        rows = out[n * 2 * KR : (n + 1) * 2 * KR]
        result.append(rows[:, :C] + sign * half_turn(rows[:, C:]))
    return result


def sections(q, recv, work1, work2, g_low, g_high, ret_send):
    def forward_z(h, carry):
        blocks = hadamard([recv[q, h * NZ + z].astype(F32) for z in range(NZ)])
        for t in range(NZ):
            work1[h, t] = blocks[t]
        return carry

    def forward_h(t, carry):
        blocks = times_gate(hadamard([work1[h, t] for h in range(NH)]), g_low[t])
        for h in range(NH):
            work2[h, t] = blocks[h]
        return carry

    def inverse_z(h, carry):
        blocks = hadamard(times_gate([work2[h, t] for t in range(NZ)], g_high[h]))
        for z in range(NZ):
            work1[h, z] = blocks[z]
        return carry

    def inverse_h(z, carry):
        blocks = hadamard([work1[t, z] for t in range(NH)])
        for h in range(NH):
            ret_send[q, h, z] = (blocks[h] * (1.0 / GROUP)).astype(BF16)
        return carry

    lax.fori_loop(0, NH, forward_z, 0, unroll=UNROLL)
    lax.fori_loop(0, NZ, forward_h, 0, unroll=UNROLL)
    lax.fori_loop(0, NH, inverse_z, 0, unroll=UNROLL)
    lax.fori_loop(0, NZ, inverse_h, 0, unroll=UNROLL)


def unit(turn):
    turn = lax.rem(turn, 4)
    odd = lax.rem(turn, 2)
    return ((1 - odd) * (1 - turn)).astype(F32), (odd * (2 - turn)).astype(F32)


def assemble(gathered, out_ref):
    lane = lax.broadcasted_iota(jnp.int32, (NZ, 128), 1) // AMP
    for part in range(2):
        for y_hi in range(2):
            for x_hi in range(2):
                total = None
                for x_lo in range(2):
                    for y_lo in range(2):
                        for core in range(2):
                            source = part * 4 + x_hi * 2 + x_lo
                            target = x_lo * 4 + y_lo * 2 + core
                            rows = gathered[y_hi + 2 * core + 4 * y_lo]
                            shift = (target - source) * AMP % 128
                            moved = pltpu.roll(rows, shift, 1) if shift else rows
                            total = moved if total is None else jnp.where(lane == target, moved, total)
                for z in range(NZ):
                    group = (y_hi * NZ + z) * 2 + x_hi
                    out_ref[part : part + 1, group * 128 : (group + 1) * 128] = total[z : z + 1]


def kernel(
    x_ref, gates_ref, rows_ref, cols_ref, out_ref,
    x_in, staged, recv, work1, work2, ret_send, ret, gates, right, tops, g_low, g_high, g_x,
    cols, crx, ccx, left, wbuf, finz, finx, finh,
    local_sem, main_send, main_recv, small_send, small_recv, x_send, x_recv, back_send, back_recv, fin_send, fin_recv, ready,
):
    mz, my, mx, mc = position()
    mh = bits_index(my, mc)
    mine = mh * NZ + mz
    z0, z1, z2 = lax.rem(mz, 2), lax.rem(mz // 2, 2), mz // 4
    h_ones = my // 2 + lax.rem(my, 2) + mc

    z_peers = [lax.rem(mz + d, NZ) for d in range(NZ)]
    y_peers = [lax.rem(my + d, NY) for d in range(NY)]
    c_peers = [lax.rem(mc + d, NC) for d in range(NC)]
    x_peers = [lax.rem(mx + d, NX) for d in range(NX)]
    crossing = [(dx, dy, dc) for dx in Y_ORDER for dy in Y_ORDER for dc in range(NC) if dx or dy or dc]
    crossing.sort(key=lambda d: -min(d[0], 4 - d[0]) - min(d[1], 4 - d[1]))
    back = [(dy, dc) for dy in Y_ORDER for dc in range(NC) if dy or dc]

    x_copy = pltpu.make_async_copy(x_ref, x_in, local_sem.at[3])
    x_copy.start()
    cols_copy = pltpu.make_async_copy(cols_ref, cols, local_sem.at[1])
    cols_copy.start()
    own_rows = pltpu.make_async_copy(rows_ref.at[:, :, pl.ds(pl.multiple_of(mz * 128, 128), 128)], crx.at[mx, mz], local_sem.at[2])
    own_rows.start()
    gates_copy = pltpu.make_async_copy(gates_ref, gates, local_sem.at[0])
    gates_copy.start()

    barrier = pltpu.get_barrier_semaphore()
    near = [(mz, y_peers[dy], mx, c_peers[dc]) for dy, dc in back]
    near += [(z_peers[dz], my, mx, mc) for dz in (1, NZ - 1)]
    near += [(mz, my, x_peers[dx], mc) for dx in range(1, NX)]
    for there in near:
        pl.semaphore_signal(barrier, inc=1, device_id=device(*there), device_id_type=MESH)

    cos, sin = unit(z0 + z1 + z2 + h_ones)
    low = lax.broadcasted_iota(jnp.int32, (2 * KR, C), 0) < KR

    def stage(target, carry):
        re = x_in[0, target].astype(F32)
        im = x_in[1, target].astype(F32)
        re, im = cos * re - sin * im, cos * im + sin * re
        for half in range(2):
            a, b = re[8 * half : 8 * half + 8], im[8 * half : 8 * half + 8]
            staged[2 * half, target] = jnp.where(low, a, half_turn(b)).astype(BF16)
            staged[2 * half + 1, target] = jnp.where(low, half_turn(a), b).astype(BF16)
        return carry

    cols_copy.wait()
    ccx[mx, mz] = cols[...].astype(BF16)
    x_copy.wait()
    lax.fori_loop(0, GROUP, stage, 0, unroll=4)
    for q in range(CHUNKS):
        recv[q, mine] = staged[q, mz * NH + mh]
    pl.semaphore_wait(barrier, len(near))

    def remote(src, dst, send, recv_sem, where):
        copy = pltpu.make_async_remote_copy(
            src_ref=src, dst_ref=dst, send_sem=send, recv_sem=recv_sem, device_id=device(*where), device_id_type=MESH
        )
        copy.start()

    def send_rows(dz):
        pz = z_peers[dz]
        columns = pl.ds(pl.multiple_of(pz * 128, 128), 128)
        remote(rows_ref.at[:, :, columns], crx.at[mx, mz], small_send.at[0], small_recv.at[0], (pz, my, mx, mc))

    def send_columns(origin, dz, which):
        slot = ccx.at[mx, z_peers[origin]]
        remote(slot, slot, small_send.at[which], small_recv.at[which], (z_peers[dz], my, mx, mc))

    def send_tensor(q, dz):
        for dy in Y_ORDER:
            for dc in range(NC):
                if dz or dy or dc:
                    pz, py, pc = z_peers[dz], y_peers[dy], c_peers[dc]
                    block = pz * NH + bits_index(py, pc)
                    remote(staged.at[q, block], recv.at[q, mine], main_send.at[q], main_recv.at[q], (pz, py, mx, pc))

    send_tensor(0, 0)
    for level in range(4):
        pl.semaphore_signal(ready.at[level, 0], inc=1, device_id=device(z_peers[1], my, mx, mc), device_id_type=MESH)
        pl.semaphore_signal(ready.at[level, 1], inc=1, device_id=device(z_peers[7], my, mx, mc), device_id_type=MESH)
        distances = (level + 1, NZ - level - 1) if level < 3 else (4,)
        for dz in distances:
            send_rows(dz)
            send_columns(0, dz, 1)
        pl.semaphore_wait(ready.at[level, 0], 1)
        pl.semaphore_wait(ready.at[level, 1], 1)
        for dz in distances:
            send_tensor(0, dz)
    for dz in Z_ORDER:
        send_tensor(1, dz)

    for q in range(2, CHUNKS):
        for dz in Z_ORDER:
            send_tensor(q, dz)

    gates_copy.wait()
    triple_products(gates, 0, right, tops, g_low)
    triple_products(gates, 3, right, tops, g_high)
    pair_products(gates, 6, right, tops, g_x)

    own_rows.wait()
    wait_bytes(crx.at[0, pl.ds(0, NZ - 1)], small_recv.at[0])
    wait_bytes(ccx.at[0, pl.ds(0, 7)], small_recv.at[1])
    for dx in (2, 1, 3):
        there = (mz, my, x_peers[dx], mc)
        remote(crx.at[mx], crx.at[mx], x_send.at[0], x_recv.at[0], there)
        remote(ccx.at[mx], ccx.at[mx], x_send.at[1], x_recv.at[1], there)

    def closing_rows_in_order():
        row = lax.broadcasted_iota(jnp.int32, (128, 2 * C), 0)
        column = lax.broadcasted_iota(jnp.int32, (128, 2 * C), 1)
        wanted = (row // KR) * 2 * KR + lax.rem(row, KR)
        wanted = jnp.where(column < C, wanted, wanted + C + KR)
        select = jnp.where(column == wanted, 1.0, 0.0).astype(BF16)
        for z in range(NZ):
            rows = [crx[xs, z, part] for part in range(2) for xs in range(NX)]
            out = jnp.dot(jnp.concatenate(rows, axis=0), select, preferred_element_type=F32)
            half = NX * AMP
            for_re = out[:half, :C] - out[half:, C:]
            for_im = out[half:, :C] + out[:half, C:]
            left[z] = jnp.concatenate([for_re, for_im], axis=0).astype(BF16)

    def columns_through_x():
        m0, m1 = lax.rem(mx, 2), mx // 2
        for xs in range(NX):
            parts = []
            for z in range(NZ):
                both = ccx[xs, z]
                parts.append(jnp.concatenate([both[0], -both[1]], axis=1))
            vectors = jnp.concatenate(parts, axis=0)
            s0, s1 = xs % 2, xs // 2
            e0 = s0 + m0 - 2 * s0 * m0
            e1 = s1 + m1 - 2 * s1 * m1
            f0 = (1 - 2 * e0).astype(F32)
            f1 = (1 - 2 * e1).astype(F32)
            cos, sin = unit(m0 + m1 - s0 - s1 - h_ones + 8)
            total = None
            for t in range(4):
                u = lax.dot_general(vectors, g_x[t], (((1,), (1,)), ((), ())), preferred_element_type=F32)
                if t & 1:
                    u = u * f0
                if t & 2:
                    u = u * f1
                total = u if total is None else total + u
            re, neg = total[:, :C], total[:, C:]
            re, neg = cos * re + sin * neg, cos * neg - sin * re
            for z in range(NZ):
                a, b = re[z * AMP : (z + 1) * AMP], neg[z * AMP : (z + 1) * AMP]
                a, b = ((a, b), (-b, a), (-a, -b), (b, -a))[ones(z)]
                wbuf[z, xs * AMP : (xs + 1) * AMP, :C] = a
                wbuf[z, xs * AMP : (xs + 1) * AMP, C:] = b

    for q in range(CHUNKS):
        wait_bytes(recv.at[q, pl.ds(0, GROUP - 1)], main_recv.at[q])
        sections(q, recv, work1, work2, g_low, g_high, ret_send)
        for dy, dc in back:
            py, pc = y_peers[dy], c_peers[dc]
            remote(ret_send.at[q, bits_index(py, pc)], ret.at[q, mh], back_send.at[q], back_recv.at[q], (mz, py, mx, pc))
        ret[q, mh] = ret_send[q, mh]
        if q == 0:
            wait_bytes(crx.at[pl.ds(0, NX - 1)], x_recv.at[0])
            wait_bytes(ccx.at[pl.ds(0, NX - 1)], x_recv.at[1])
            closing_rows_in_order()
            columns_through_x()

    for q in range(CHUNKS):
        wait_bytes(ret.at[q, pl.ds(0, NH - 1)], back_recv.at[q])

    def close(z, carry):
        blocks = []
        for h in range(NH):
            for q in range(CHUNKS):
                blocks.append(ret[q, h, z].astype(F32))
        tensor = jnp.concatenate(blocks, axis=0).astype(BF16)
        proj = jnp.dot(left[z], tensor, preferred_element_type=F32)
        half = NX * AMP
        p_re, p_im = proj[:half], proj[half:]
        w = wbuf[z]
        w_re, w_neg = w[:, :C], w[:, C:]
        a_re = p_re * w_re + p_im * w_neg
        a_im = p_im * w_re - p_re * w_neg
        both = jnp.concatenate([a_re[:, :128] + a_re[:, 128:], a_im[:, :128] + a_im[:, 128:]], axis=0)
        finz[mz, pl.ds(z, 1)] = jnp.sum(jnp.transpose(both), axis=0, keepdims=True)
        return carry

    lax.fori_loop(0, NZ, close, 0, unroll=UNROLL)

    for dz in Z_ORDER[:-1]:
        remote(finz.at[mz], finz.at[mz], fin_send.at[0], fin_recv.at[0], (z_peers[dz], my, mx, mc))
    wait_bytes(crx.at[0, pl.ds(0, NZ - 1)], small_send.at[0])
    wait_bytes(ccx.at[0, pl.ds(0, 7)], small_send.at[1])
    wait_bytes(crx.at[pl.ds(0, NX - 1)], x_send.at[0])
    wait_bytes(ccx.at[pl.ds(0, NX - 1)], x_send.at[1])
    for q in range(CHUNKS):
        wait_bytes(recv.at[q, pl.ds(0, GROUP - 1)], main_send.at[q])
        wait_bytes(ret.at[q, pl.ds(0, NH - 1)], back_send.at[q])
    wait_bytes(finz.at[pl.ds(0, NZ - 1)], fin_recv.at[0])
    finx[mx * NH + mh] = jnp.sum(finz[...], axis=0)
    for dx, dy, dc in crossing:
        there = (mz, y_peers[dy], x_peers[dx], c_peers[dc])
        remote(finx.at[mx * NH + mh], finx.at[mx * NH + mh], fin_send.at[1], fin_recv.at[1], there)
    wait_bytes(finz.at[pl.ds(0, NZ - 1)], fin_send.at[0])
    wait_bytes(finx.at[pl.ds(0, NX * NH - 1)], fin_recv.at[1])
    finh[...] = jnp.sum(finx[...].reshape(NX, NH, NZ, 128), axis=0)
    assemble(finh, out_ref)
    wait_bytes(finx.at[pl.ds(0, NX * NH - 1)], fin_send.at[1])


def local(tensors, gates, closing_rows, closing_columns):
    dma = pltpu.SemaphoreType.DMA
    out = pl.pallas_call(
        kernel,
        out_shape=jax.ShapeDtypeStruct((2, NZ * NH * NX * AMP), F32),
        in_specs=[pl.BlockSpec(memory_space=pl.ANY)] * 4,
        out_specs=pl.BlockSpec(memory_space=pltpu.VMEM),
        scratch_shapes=[
            pltpu.VMEM((2, GROUP, 16, C), BF16),
            pltpu.VMEM((CHUNKS, GROUP, 2 * KR, C), BF16),
            pltpu.VMEM((CHUNKS, GROUP, 2 * KR, C), BF16),
            pltpu.VMEM((NH, NZ, 2 * KR, C), F32),
            pltpu.VMEM((NH, NZ, 2 * KR, C), F32),
            pltpu.VMEM((CHUNKS, NH, NZ, 2 * KR, C), BF16),
            pltpu.VMEM((CHUNKS, NH, NZ, 2 * KR, C), BF16),
            pltpu.VMEM((8, 2, 2, C, C), BF16),
            pltpu.VMEM((2, 2 * C, 2 * C), BF16),
            pltpu.VMEM((6, C, 2 * C), BF16),
            pltpu.VMEM((8, C, 2 * C), BF16),
            pltpu.VMEM((8, C, 2 * C), BF16),
            pltpu.VMEM((4, 2 * C, 2 * C), BF16),
            pltpu.VMEM((2, AMP, C), F32),
            pltpu.VMEM((NX, NZ, 2, AMP, 128), BF16),
            pltpu.VMEM((NX, NZ, 2, AMP, C), BF16),
            pltpu.VMEM((NZ, 128, C), BF16),
            pltpu.VMEM((NZ, NX * AMP, 2 * C), F32),
            pltpu.VMEM((NZ, NZ, 128), F32),
            pltpu.VMEM((NX * NH, NZ, 128), F32),
            pltpu.VMEM((NH, NZ, 128), F32),
            dma((4,)),
            dma((CHUNKS,)),
            dma((CHUNKS,)),
            dma((3,)),
            dma((3,)),
            dma((2,)),
            dma((2,)),
            dma((CHUNKS,)),
            dma((CHUNKS,)),
            dma((2,)),
            dma((2,)),
            pltpu.SemaphoreType.REGULAR((4, 2)),
        ],
        compiler_params=pltpu.CompilerParams(
            collective_id=0, has_side_effects=True, vmem_limit_bytes=56 * 1024 * 1024
        ),
        name="network",
    )(tensors.reshape(2, GROUP, 16, C), gates, closing_rows, closing_columns)
    return out * (1.0 / NX)


def solution(mesh):
    placed = (
        P(None, "sx", "sy", None, None),
        P(),
        P(None, ("sx", "sy"), None),
        P(None, ("sx", "sy"), None),
    )
    return jax.shard_map(local, mesh=mesh, in_specs=placed, out_specs=P(), check_vma=False)
```

```python
import functools

import jax
import jax.numpy as jnp
from jax import lax
from jax.experimental import pallas as pl
from jax.experimental.pallas import tpu as pltpu
from jax.sharding import PartitionSpec as P

MESH = pl.DeviceIdType.MESH
F32 = jnp.float32
BF16 = jnp.bfloat16
NZ, NY, NX, NC = 8, 4, 4, 2
NH = NY * NC
GROUP = NZ * NH
C = 256
CHUNKS = 4
KR = 4
UNROLL = True
AMP = 16
Z_ORDER = (4, 3, 5, 2, 6, 1, 7, 0)
Y_ORDER = (2, 1, 3, 0)


def position():
    sx = lax.axis_index("sx")
    sy = lax.axis_index("sy")
    return lax.rem(sx, 8), (sx // 8) * 2 + lax.rem(sy // 2, 2), sy // 4, lax.rem(sy, 2)


def device(z, y, x, c):
    return ((y // 2) * 8 + z, x * 4 + lax.rem(y, 2) * 2 + c)


def bits_index(y, c):
    return y // 2 + 2 * c + 4 * lax.rem(y, 2)


def ones(number):
    return bin(number).count("1")


def turned(block, power):
    power %= 4
    re, im = block[:, :C], block[:, C:]
    if power == 0:
        return block
    if power == 1:
        return jnp.concatenate([-im, re], axis=1)
    if power == 2:
        return -block
    return jnp.concatenate([im, -re], axis=1)


def hadamard(blocks):
    blocks = list(blocks)
    half = 1
    while half < len(blocks):
        for low in range(len(blocks)):
            if not low & half:
                a, b = blocks[low], blocks[low | half]
                blocks[low], blocks[low | half] = a + b, a - b
        half *= 2
    return blocks


def fill_full(full, index, re, im):
    full[index, :C, :C] = re
    full[index, :C, C:] = im
    full[index, C:, :C] = -im
    full[index, C:, C:] = re


def section_pairs(gates, first, right, tops):
    for which in range(2):
        tops[which, :, :C] = gates[first, which, 0]
        tops[which, :, C:] = gates[first, which, 1]
        fill_full(right, which, gates[first + 1, which, 0], gates[first + 1, which, 1])
    aa = jnp.dot(tops[0], right[0], preferred_element_type=F32)
    bb = jnp.dot(tops[1], right[1], preferred_element_type=F32)
    even, odd = aa - bb, aa + bb
    ba = jnp.dot(tops[1], right[0], preferred_element_type=F32)
    ab = jnp.dot(tops[0], right[1], preferred_element_type=F32)
    plus, minus = turned(ba + ab, -1), turned(ba - ab, -1)
    return even + plus, odd - minus, odd + minus, even - plus


def triple_products(gates, first, right, tops, full):
    for low, pair in enumerate(section_pairs(gates, first, right, tops)):
        tops[2 + low] = pair.astype(BF16)
    for which in range(2):
        fill_full(right, which, gates[first + 2, which, 0], gates[first + 2, which, 1])
    for low in range(4):
        with_a = jnp.dot(tops[2 + low], right[0], preferred_element_type=F32)
        with_b = turned(jnp.dot(tops[2 + low], right[1], preferred_element_type=F32), -1)
        for third, out in enumerate((with_a + with_b, with_a - with_b)):
            out = out.astype(BF16)
            full[low + 4 * third] = out


def pair_products(gates, first, right, tops, full):
    for low, pair in enumerate(section_pairs(gates, first, right, tops)):
        pair = pair.astype(BF16)
        fill_full(full, low, pair[:, :C], pair[:, C:])


def wait_bytes(ref, sem):
    pltpu.make_async_copy(ref, ref, sem).wait()


def half_turn(block):
    return pltpu.roll(block, KR, 0)


def times_gate(blocks, gate):
    left = jnp.concatenate(blocks, axis=0).astype(BF16)
    out = jnp.dot(left, gate, preferred_element_type=F32)
    sign = jnp.where(lax.broadcasted_iota(jnp.int32, (2 * KR, C), 0) < KR, -1.0, 1.0)
    result = []
    for n in range(len(blocks)):
        rows = out[n * 2 * KR : (n + 1) * 2 * KR]
        result.append(rows[:, :C] + sign * half_turn(rows[:, C:]))
    return result


def sections(q, recv, work1, work2, g_low, g_high, ret_send):
    def forward_z(h, carry):
        blocks = hadamard([recv[q, h * NZ + z].astype(F32) for z in range(NZ)])
        for t in range(NZ):
            work1[h, t] = blocks[t]
        return carry

    def forward_h(t, carry):
        blocks = times_gate(hadamard([work1[h, t] for h in range(NH)]), g_low[t])
        for h in range(NH):
            work2[h, t] = blocks[h]
        return carry

    def inverse_z(h, carry):
        blocks = hadamard(times_gate([work2[h, t] for t in range(NZ)], g_high[h]))
        for z in range(NZ):
            work1[h, z] = blocks[z]
        return carry

    def inverse_h(z, carry):
        blocks = hadamard([work1[t, z] for t in range(NH)])
        for h in range(NH):
            ret_send[q, h, z] = (blocks[h] * (1.0 / GROUP)).astype(BF16)
        return carry

    lax.fori_loop(0, NH, forward_z, 0, unroll=UNROLL)
    lax.fori_loop(0, NZ, forward_h, 0, unroll=UNROLL)
    lax.fori_loop(0, NH, inverse_z, 0, unroll=UNROLL)
    lax.fori_loop(0, NZ, inverse_h, 0, unroll=UNROLL)


def unit(turn):
    turn = lax.rem(turn, 4)
    odd = lax.rem(turn, 2)
    return ((1 - odd) * (1 - turn)).astype(F32), (odd * (2 - turn)).astype(F32)


def assemble(gathered, out_ref):
    lane = lax.broadcasted_iota(jnp.int32, (NZ, 128), 1) // AMP
    for part in range(2):
        for y_hi in range(2):
            for x_hi in range(2):
                total = None
                for x_lo in range(2):
                    for y_lo in range(2):
                        for core in range(2):
                            source = part * 4 + x_hi * 2 + x_lo
                            target = x_lo * 4 + y_lo * 2 + core
                            rows = gathered[y_hi + 2 * core + 4 * y_lo]
                            shift = (target - source) * AMP % 128
                            moved = pltpu.roll(rows, shift, 1) if shift else rows
                            total = moved if total is None else jnp.where(lane == target, moved, total)
                for z in range(NZ):
                    group = (y_hi * NZ + z) * 2 + x_hi
                    out_ref[part : part + 1, group * 128 : (group + 1) * 128] = total[z : z + 1]


def kernel(
    x_ref, gates_ref, rows_ref, cols_ref, out_ref,
    x_in, staged, recv, work1, work2, ret_send, ret, gates, right, tops, g_low, g_high, g_x,
    cols, crx, ccx, left, wbuf, finz, finx, finh,
    local_sem, main_send, main_recv, small_send, small_recv, x_send, x_recv, back_send, back_recv, fin_send, fin_recv, ready,
):
    mz, my, mx, mc = position()
    mh = bits_index(my, mc)
    mine = mh * NZ + mz
    z0, z1, z2 = lax.rem(mz, 2), lax.rem(mz // 2, 2), mz // 4
    h_ones = my // 2 + lax.rem(my, 2) + mc

    z_peers = [lax.rem(mz + d, NZ) for d in range(NZ)]
    y_peers = [lax.rem(my + d, NY) for d in range(NY)]
    c_peers = [lax.rem(mc + d, NC) for d in range(NC)]
    x_peers = [lax.rem(mx + d, NX) for d in range(NX)]
    crossing = [(dx, dy, dc) for dx in Y_ORDER for dy in Y_ORDER for dc in range(NC) if dx or dy or dc]
    crossing.sort(key=lambda d: -min(d[0], 4 - d[0]) - min(d[1], 4 - d[1]))
    back = [(dy, dc) for dy in Y_ORDER for dc in range(NC) if dy or dc]

    x_copy = pltpu.make_async_copy(x_ref, x_in, local_sem.at[3])
    x_copy.start()
    cols_copy = pltpu.make_async_copy(cols_ref, cols, local_sem.at[1])
    cols_copy.start()
    own_rows = pltpu.make_async_copy(rows_ref.at[:, :, pl.ds(pl.multiple_of(mz * 128, 128), 128)], crx.at[mx, mz], local_sem.at[2])
    own_rows.start()
    gates_copy = pltpu.make_async_copy(gates_ref, gates, local_sem.at[0])
    gates_copy.start()

    barrier = pltpu.get_barrier_semaphore()
    near = [(mz, y_peers[dy], mx, c_peers[dc]) for dy, dc in back]
    near += [(z_peers[dz], my, mx, mc) for dz in (1, NZ - 1)]
    near += [(mz, my, x_peers[dx], mc) for dx in range(1, NX)]
    for there in near:
        pl.semaphore_signal(barrier, inc=1, device_id=device(*there), device_id_type=MESH)

    cos, sin = unit(z0 + z1 + z2 + h_ones)
    low = lax.broadcasted_iota(jnp.int32, (2 * KR, C), 0) < KR

    def stage(target, carry):
        re = x_in[0, target].astype(F32)
        im = x_in[1, target].astype(F32)
        re, im = cos * re - sin * im, cos * im + sin * re
        for half in range(2):
            a, b = re[8 * half : 8 * half + 8], im[8 * half : 8 * half + 8]
            staged[2 * half, target] = jnp.where(low, a, half_turn(b)).astype(BF16)
            staged[2 * half + 1, target] = jnp.where(low, half_turn(a), b).astype(BF16)
        return carry

    cols_copy.wait()
    ccx[mx, mz] = cols[...].astype(BF16)
    x_copy.wait()
    lax.fori_loop(0, GROUP, stage, 0, unroll=4)
    for q in range(CHUNKS):
        recv[q, mine] = staged[q, mz * NH + mh]
    pl.semaphore_wait(barrier, len(near))

    def remote(src, dst, send, recv_sem, where):
        copy = pltpu.make_async_remote_copy(
            src_ref=src, dst_ref=dst, send_sem=send, recv_sem=recv_sem, device_id=device(*where), device_id_type=MESH
        )
        copy.start()

    def send_rows(dz):
        pz = z_peers[dz]
        columns = pl.ds(pl.multiple_of(pz * 128, 128), 128)
        remote(rows_ref.at[:, :, columns], crx.at[mx, mz], small_send.at[0], small_recv.at[0], (pz, my, mx, mc))

    def send_columns(origin, dz, which):
        slot = ccx.at[mx, z_peers[origin]]
        remote(slot, slot, small_send.at[which], small_recv.at[which], (z_peers[dz], my, mx, mc))

    def send_tensor(q, dz):
        for dy in Y_ORDER:
            for dc in range(NC):
                if dz or dy or dc:
                    pz, py, pc = z_peers[dz], y_peers[dy], c_peers[dc]
                    block = pz * NH + bits_index(py, pc)
                    remote(staged.at[q, block], recv.at[q, mine], main_send.at[q], main_recv.at[q], (pz, py, mx, pc))

    send_tensor(0, 0)
    for level in range(4):
        pl.semaphore_signal(ready.at[level, 0], inc=1, device_id=device(z_peers[1], my, mx, mc), device_id_type=MESH)
        pl.semaphore_signal(ready.at[level, 1], inc=1, device_id=device(z_peers[7], my, mx, mc), device_id_type=MESH)
        distances = (level + 1, NZ - level - 1) if level < 3 else (4,)
        for dz in distances:
            send_rows(dz)
            if level == 0:
                send_columns(0, dz, 2)
            if level == 1:
                send_columns(0, dz, 1)
        if level == 3:
            wait_bytes(ccx.at[0, pl.ds(0, 2)], small_recv.at[1])
            for origin, dz in ((6, 2), (6, 1), (2, 7)):
                send_columns(origin, dz, 2)
        pl.semaphore_wait(ready.at[level, 0], 1)
        pl.semaphore_wait(ready.at[level, 1], 1)
        for dz in distances:
            send_tensor(0, dz)
    for dz in Z_ORDER:
        send_tensor(1, dz)

    for q in range(2, CHUNKS):
        for dz in Z_ORDER:
            send_tensor(q, dz)

    gates_copy.wait()
    triple_products(gates, 0, right, tops, g_low)
    triple_products(gates, 3, right, tops, g_high)
    pair_products(gates, 6, right, tops, g_x)

    own_rows.wait()
    wait_bytes(crx.at[0, pl.ds(0, NZ - 1)], small_recv.at[0])
    wait_bytes(ccx.at[0, pl.ds(0, 5)], small_recv.at[2])
    for dx in (2, 1, 3):
        there = (mz, my, x_peers[dx], mc)
        remote(crx.at[mx], crx.at[mx], x_send.at[0], x_recv.at[0], there)
        remote(ccx.at[mx], ccx.at[mx], x_send.at[1], x_recv.at[1], there)

    def closing_rows_in_order():
        row = lax.broadcasted_iota(jnp.int32, (128, 2 * C), 0)
        column = lax.broadcasted_iota(jnp.int32, (128, 2 * C), 1)
        wanted = (row // KR) * 2 * KR + lax.rem(row, KR)
        wanted = jnp.where(column < C, wanted, wanted + C + KR)
        select = jnp.where(column == wanted, 1.0, 0.0).astype(BF16)
        for z in range(NZ):
            rows = [crx[xs, z, part] for part in range(2) for xs in range(NX)]
            out = jnp.dot(jnp.concatenate(rows, axis=0), select, preferred_element_type=F32)
            half = NX * AMP
            for_re = out[:half, :C] - out[half:, C:]
            for_im = out[half:, :C] + out[:half, C:]
            left[z] = jnp.concatenate([for_re, for_im], axis=0).astype(BF16)

    def columns_through_x():
        m0, m1 = lax.rem(mx, 2), mx // 2
        for xs in range(NX):
            parts = []
            for z in range(NZ):
                both = ccx[xs, z]
                parts.append(jnp.concatenate([both[0], -both[1]], axis=1))
            vectors = jnp.concatenate(parts, axis=0)
            s0, s1 = xs % 2, xs // 2
            e0 = s0 + m0 - 2 * s0 * m0
            e1 = s1 + m1 - 2 * s1 * m1
            f0 = (1 - 2 * e0).astype(F32)
            f1 = (1 - 2 * e1).astype(F32)
            cos, sin = unit(m0 + m1 - s0 - s1 - h_ones + 8)
            total = None
            for t in range(4):
                u = lax.dot_general(vectors, g_x[t], (((1,), (1,)), ((), ())), preferred_element_type=F32)
                if t & 1:
                    u = u * f0
                if t & 2:
                    u = u * f1
                total = u if total is None else total + u
            re, neg = total[:, :C], total[:, C:]
            re, neg = cos * re + sin * neg, cos * neg - sin * re
            for z in range(NZ):
                a, b = re[z * AMP : (z + 1) * AMP], neg[z * AMP : (z + 1) * AMP]
                a, b = ((a, b), (-b, a), (-a, -b), (b, -a))[ones(z)]
                wbuf[z, xs * AMP : (xs + 1) * AMP, :C] = a
                wbuf[z, xs * AMP : (xs + 1) * AMP, C:] = b

    for q in range(CHUNKS):
        wait_bytes(recv.at[q, pl.ds(0, GROUP - 1)], main_recv.at[q])
        sections(q, recv, work1, work2, g_low, g_high, ret_send)
        for dy, dc in back:
            py, pc = y_peers[dy], c_peers[dc]
            remote(ret_send.at[q, bits_index(py, pc)], ret.at[q, mh], back_send.at[q], back_recv.at[q], (mz, py, mx, pc))
        ret[q, mh] = ret_send[q, mh]

    wait_bytes(crx.at[pl.ds(0, NX - 1)], x_recv.at[0])
    wait_bytes(ccx.at[pl.ds(0, NX - 1)], x_recv.at[1])
    closing_rows_in_order()
    columns_through_x()

    for q in range(CHUNKS):
        wait_bytes(ret.at[q, pl.ds(0, NH - 1)], back_recv.at[q])

    def close(z, carry):
        blocks = []
        for h in range(NH):
            for q in range(CHUNKS):
                blocks.append(ret[q, h, z].astype(F32))
        tensor = jnp.concatenate(blocks, axis=0).astype(BF16)
        proj = jnp.dot(left[z], tensor, preferred_element_type=F32)
        half = NX * AMP
        p_re, p_im = proj[:half], proj[half:]
        w = wbuf[z]
        w_re, w_neg = w[:, :C], w[:, C:]
        a_re = p_re * w_re + p_im * w_neg
        a_im = p_im * w_re - p_re * w_neg
        both = jnp.concatenate([a_re[:, :128] + a_re[:, 128:], a_im[:, :128] + a_im[:, 128:]], axis=0)
        finz[mz, pl.ds(z, 1)] = jnp.sum(jnp.transpose(both), axis=0, keepdims=True)
        return carry

    lax.fori_loop(0, NZ, close, 0, unroll=UNROLL)

    for dz in Z_ORDER[:-1]:
        remote(finz.at[mz], finz.at[mz], fin_send.at[0], fin_recv.at[0], (z_peers[dz], my, mx, mc))
    wait_bytes(crx.at[0, pl.ds(0, NZ - 1)], small_send.at[0])
    wait_bytes(ccx.at[0, pl.ds(0, 2)], small_send.at[1])
    wait_bytes(ccx.at[0, pl.ds(0, 5)], small_send.at[2])
    wait_bytes(crx.at[pl.ds(0, NX - 1)], x_send.at[0])
    wait_bytes(ccx.at[pl.ds(0, NX - 1)], x_send.at[1])
    for q in range(CHUNKS):
        wait_bytes(recv.at[q, pl.ds(0, GROUP - 1)], main_send.at[q])
        wait_bytes(ret.at[q, pl.ds(0, NH - 1)], back_send.at[q])
    wait_bytes(finz.at[pl.ds(0, NZ - 1)], fin_recv.at[0])
    finx[mx * NH + mh] = jnp.sum(finz[...], axis=0)
    for dx, dy, dc in crossing:
        there = (mz, y_peers[dy], x_peers[dx], c_peers[dc])
        remote(finx.at[mx * NH + mh], finx.at[mx * NH + mh], fin_send.at[1], fin_recv.at[1], there)
    wait_bytes(finz.at[pl.ds(0, NZ - 1)], fin_send.at[0])
    wait_bytes(finx.at[pl.ds(0, NX * NH - 1)], fin_recv.at[1])
    finh[...] = jnp.sum(finx[...].reshape(NX, NH, NZ, 128), axis=0)
    assemble(finh, out_ref)
    wait_bytes(finx.at[pl.ds(0, NX * NH - 1)], fin_send.at[1])


def local(tensors, gates, closing_rows, closing_columns):
    dma = pltpu.SemaphoreType.DMA
    out = pl.pallas_call(
        kernel,
        out_shape=jax.ShapeDtypeStruct((2, NZ * NH * NX * AMP), F32),
        in_specs=[pl.BlockSpec(memory_space=pl.ANY)] * 4,
        out_specs=pl.BlockSpec(memory_space=pltpu.VMEM),
        scratch_shapes=[
            pltpu.VMEM((2, GROUP, 16, C), BF16),
            pltpu.VMEM((CHUNKS, GROUP, 2 * KR, C), BF16),
            pltpu.VMEM((CHUNKS, GROUP, 2 * KR, C), BF16),
            pltpu.VMEM((NH, NZ, 2 * KR, C), F32),
            pltpu.VMEM((NH, NZ, 2 * KR, C), F32),
            pltpu.VMEM((CHUNKS, NH, NZ, 2 * KR, C), BF16),
            pltpu.VMEM((CHUNKS, NH, NZ, 2 * KR, C), BF16),
            pltpu.VMEM((8, 2, 2, C, C), BF16),
            pltpu.VMEM((2, 2 * C, 2 * C), BF16),
            pltpu.VMEM((6, C, 2 * C), BF16),
            pltpu.VMEM((8, C, 2 * C), BF16),
            pltpu.VMEM((8, C, 2 * C), BF16),
            pltpu.VMEM((4, 2 * C, 2 * C), BF16),
            pltpu.VMEM((2, AMP, C), F32),
            pltpu.VMEM((NX, NZ, 2, AMP, 128), BF16),
            pltpu.VMEM((NX, NZ, 2, AMP, C), BF16),
            pltpu.VMEM((NZ, 128, C), BF16),
            pltpu.VMEM((NZ, NX * AMP, 2 * C), F32),
            pltpu.VMEM((NZ, NZ, 128), F32),
            pltpu.VMEM((NX * NH, NZ, 128), F32),
            pltpu.VMEM((NH, NZ, 128), F32),
            dma((4,)),
            dma((CHUNKS,)),
            dma((CHUNKS,)),
            dma((3,)),
            dma((3,)),
            dma((2,)),
            dma((2,)),
            dma((CHUNKS,)),
            dma((CHUNKS,)),
            dma((2,)),
            dma((2,)),
            pltpu.SemaphoreType.REGULAR((4, 2)),
        ],
        compiler_params=pltpu.CompilerParams(
            collective_id=0, has_side_effects=True, vmem_limit_bytes=56 * 1024 * 1024
        ),
        name="network",
    )(tensors.reshape(2, GROUP, 16, C), gates, closing_rows, closing_columns)
    return out * (1.0 / NX)


def solution(mesh):
    placed = (
        P(None, "sx", "sy", None, None),
        P(),
        P(None, ("sx", "sy"), None),
        P(None, ("sx", "sy"), None),
    )
    return jax.shard_map(local, mesh=mesh, in_specs=placed, out_specs=P(), check_vma=False)
```

```python
import functools

import jax
import jax.numpy as jnp
from jax import lax
from jax.experimental import pallas as pl
from jax.experimental.pallas import tpu as pltpu
from jax.sharding import PartitionSpec as P

MESH = pl.DeviceIdType.MESH
F32 = jnp.float32
BF16 = jnp.bfloat16
NZ, NY, NX, NC = 8, 4, 4, 2
NH = NY * NC
GROUP = NZ * NH
C = 256
CHUNKS = 4
KR = 4
UNROLL = True
AMP = 16
Z_ORDER = (4, 3, 5, 2, 6, 1, 7, 0)
Y_ORDER = (2, 1, 3, 0)


def position():
    sx = lax.axis_index("sx")
    sy = lax.axis_index("sy")
    return lax.rem(sx, 8), (sx // 8) * 2 + lax.rem(sy // 2, 2), sy // 4, lax.rem(sy, 2)


def device(z, y, x, c):
    return ((y // 2) * 8 + z, x * 4 + lax.rem(y, 2) * 2 + c)


def bits_index(y, c):
    return y // 2 + 2 * c + 4 * lax.rem(y, 2)


def ones(number):
    return bin(number).count("1")


def turned(block, power):
    power %= 4
    re, im = block[:, :C], block[:, C:]
    if power == 0:
        return block
    if power == 1:
        return jnp.concatenate([-im, re], axis=1)
    if power == 2:
        return -block
    return jnp.concatenate([im, -re], axis=1)


def hadamard(blocks):
    blocks = list(blocks)
    half = 1
    while half < len(blocks):
        for low in range(len(blocks)):
            if not low & half:
                a, b = blocks[low], blocks[low | half]
                blocks[low], blocks[low | half] = a + b, a - b
        half *= 2
    return blocks


def fill_full(full, index, re, im):
    full[index, :C, :C] = re
    full[index, :C, C:] = im
    full[index, C:, :C] = -im
    full[index, C:, C:] = re


def section_pairs(gates, first, right, tops):
    for which in range(2):
        tops[which, :, :C] = gates[first, which, 0]
        tops[which, :, C:] = gates[first, which, 1]
        fill_full(right, which, gates[first + 1, which, 0], gates[first + 1, which, 1])
    aa = jnp.dot(tops[0], right[0], preferred_element_type=F32)
    bb = jnp.dot(tops[1], right[1], preferred_element_type=F32)
    even, odd = aa - bb, aa + bb
    ba = jnp.dot(tops[1], right[0], preferred_element_type=F32)
    ab = jnp.dot(tops[0], right[1], preferred_element_type=F32)
    plus, minus = turned(ba + ab, -1), turned(ba - ab, -1)
    return even + plus, odd - minus, odd + minus, even - plus


def triple_products(gates, first, right, tops, full):
    for low, pair in enumerate(section_pairs(gates, first, right, tops)):
        tops[2 + low] = pair.astype(BF16)
    for which in range(2):
        fill_full(right, which, gates[first + 2, which, 0], gates[first + 2, which, 1])
    for low in range(4):
        with_a = jnp.dot(tops[2 + low], right[0], preferred_element_type=F32)
        with_b = turned(jnp.dot(tops[2 + low], right[1], preferred_element_type=F32), -1)
        for third, out in enumerate((with_a + with_b, with_a - with_b)):
            out = out.astype(BF16)
            full[low + 4 * third] = out


def pair_products(gates, first, right, tops, full):
    for low, pair in enumerate(section_pairs(gates, first, right, tops)):
        pair = pair.astype(BF16)
        fill_full(full, low, pair[:, :C], pair[:, C:])


def wait_bytes(ref, sem):
    pltpu.make_async_copy(ref, ref, sem).wait()


def half_turn(block):
    return pltpu.roll(block, KR, 0)


def times_gate(blocks, gate):
    left = jnp.concatenate(blocks, axis=0).astype(BF16)
    out = jnp.dot(left, gate, preferred_element_type=F32)
    sign = jnp.where(lax.broadcasted_iota(jnp.int32, (2 * KR, C), 0) < KR, -1.0, 1.0)
    result = []
    for n in range(len(blocks)):
        rows = out[n * 2 * KR : (n + 1) * 2 * KR]
        result.append(rows[:, :C] + sign * half_turn(rows[:, C:]))
    return result


def sections(q, recv, work1, work2, g_low, g_high, ret_send, send_back):
    def forward_z(h, carry):
        blocks = hadamard([recv[q, h * NZ + z].astype(F32) for z in range(NZ)])
        for t in range(NZ):
            work1[h, t] = blocks[t]
        return carry

    def forward_h(t, carry):
        blocks = times_gate(hadamard([work1[h, t] for h in range(NH)]), g_low[t])
        for h in range(NH):
            work2[h, t] = blocks[h]
        return carry

    def inverse_z(h, carry):
        blocks = hadamard(times_gate([work2[h, t] for t in range(NZ)], g_high[h]))
        for z in range(NZ):
            work1[h, z] = blocks[z]
        return carry

    def inverse_h(z, carry):
        blocks = hadamard([work1[t, z] for t in range(NH)])
        for h in range(NH):
            ret_send[q, h, z] = (blocks[h] * (1.0 / GROUP)).astype(BF16)
        return carry

    lax.fori_loop(0, NH, forward_z, 0, unroll=UNROLL)
    lax.fori_loop(0, NZ, forward_h, 0, unroll=UNROLL)
    lax.fori_loop(0, NH, inverse_z, 0, unroll=UNROLL)
    for half in range(2):
        lax.fori_loop(half * NZ // 2, (half + 1) * NZ // 2, inverse_h, 0, unroll=UNROLL)
        send_back(half)


def unit(turn):
    turn = lax.rem(turn, 4)
    odd = lax.rem(turn, 2)
    return ((1 - odd) * (1 - turn)).astype(F32), (odd * (2 - turn)).astype(F32)


def assemble(gathered, out_ref):
    lane = lax.broadcasted_iota(jnp.int32, (NZ, 128), 1) // AMP
    for part in range(2):
        for y_hi in range(2):
            for x_hi in range(2):
                total = None
                for x_lo in range(2):
                    for y_lo in range(2):
                        for core in range(2):
                            source = part * 4 + x_hi * 2 + x_lo
                            target = x_lo * 4 + y_lo * 2 + core
                            rows = gathered[y_hi + 2 * core + 4 * y_lo]
                            shift = (target - source) * AMP % 128
                            moved = pltpu.roll(rows, shift, 1) if shift else rows
                            total = moved if total is None else jnp.where(lane == target, moved, total)
                for z in range(NZ):
                    group = (y_hi * NZ + z) * 2 + x_hi
                    out_ref[part : part + 1, group * 128 : (group + 1) * 128] = total[z : z + 1]


def kernel(
    x_ref, gates_ref, rows_ref, cols_ref, out_ref,
    x_in, staged, recv, work1, work2, ret_send, ret, gates, right, tops, g_low, g_high, g_x,
    cols, crx, ccx, left, wbuf, finz, finx, finh,
    local_sem, main_send, main_recv, small_send, small_recv, x_send, x_recv, back_send, back_recv, fin_send, fin_recv, ready,
):
    mz, my, mx, mc = position()
    mh = bits_index(my, mc)
    mine = mh * NZ + mz
    z0, z1, z2 = lax.rem(mz, 2), lax.rem(mz // 2, 2), mz // 4
    h_ones = my // 2 + lax.rem(my, 2) + mc

    z_peers = [lax.rem(mz + d, NZ) for d in range(NZ)]
    y_peers = [lax.rem(my + d, NY) for d in range(NY)]
    c_peers = [lax.rem(mc + d, NC) for d in range(NC)]
    x_peers = [lax.rem(mx + d, NX) for d in range(NX)]
    crossing = [(dx, dy, dc) for dx in Y_ORDER for dy in Y_ORDER for dc in range(NC) if dx or dy or dc]
    crossing.sort(key=lambda d: -min(d[0], 4 - d[0]) - min(d[1], 4 - d[1]))
    back = [(dy, dc) for dy in Y_ORDER for dc in range(NC) if dy or dc]

    x_copy = pltpu.make_async_copy(x_ref, x_in, local_sem.at[3])
    x_copy.start()
    cols_copy = pltpu.make_async_copy(cols_ref, cols, local_sem.at[1])
    cols_copy.start()
    own_rows = pltpu.make_async_copy(rows_ref.at[:, :, pl.ds(pl.multiple_of(mz * 128, 128), 128)], crx.at[mx, mz], local_sem.at[2])
    own_rows.start()
    gates_copy = pltpu.make_async_copy(gates_ref, gates, local_sem.at[0])
    gates_copy.start()

    barrier = pltpu.get_barrier_semaphore()
    near = [(mz, y_peers[dy], mx, c_peers[dc]) for dy, dc in back]
    near += [(z_peers[dz], my, mx, mc) for dz in (1, NZ - 1)]
    near += [(mz, my, x_peers[dx], mc) for dx in range(1, NX)]
    for there in near:
        pl.semaphore_signal(barrier, inc=1, device_id=device(*there), device_id_type=MESH)

    cos, sin = unit(z0 + z1 + z2 + h_ones)
    low = lax.broadcasted_iota(jnp.int32, (2 * KR, C), 0) < KR

    def stage(target, carry):
        re = x_in[0, target].astype(F32)
        im = x_in[1, target].astype(F32)
        re, im = cos * re - sin * im, cos * im + sin * re
        for half in range(2):
            a, b = re[8 * half : 8 * half + 8], im[8 * half : 8 * half + 8]
            staged[2 * half, target] = jnp.where(low, a, half_turn(b)).astype(BF16)
            staged[2 * half + 1, target] = jnp.where(low, half_turn(a), b).astype(BF16)
        return carry

    cols_copy.wait()
    ccx[mx, mz] = cols[...].astype(BF16)
    x_copy.wait()
    lax.fori_loop(0, GROUP, stage, 0, unroll=4)
    for q in range(CHUNKS):
        recv[q, mine] = staged[q, mz * NH + mh]
    pl.semaphore_wait(barrier, len(near))

    def remote(src, dst, send, recv_sem, where):
        copy = pltpu.make_async_remote_copy(
            src_ref=src, dst_ref=dst, send_sem=send, recv_sem=recv_sem, device_id=device(*where), device_id_type=MESH
        )
        copy.start()

    def send_rows(dz):
        pz = z_peers[dz]
        columns = pl.ds(pl.multiple_of(pz * 128, 128), 128)
        remote(rows_ref.at[:, :, columns], crx.at[mx, mz], small_send.at[0], small_recv.at[0], (pz, my, mx, mc))

    def send_columns(origin, dz, which):
        slot = ccx.at[mx, z_peers[origin]]
        remote(slot, slot, small_send.at[which], small_recv.at[which], (z_peers[dz], my, mx, mc))

    def send_tensor(q, dz):
        for dy in Y_ORDER:
            for dc in range(NC):
                if dz or dy or dc:
                    pz, py, pc = z_peers[dz], y_peers[dy], c_peers[dc]
                    block = pz * NH + bits_index(py, pc)
                    remote(staged.at[q, block], recv.at[q, mine], main_send.at[q], main_recv.at[q], (pz, py, mx, pc))

    send_tensor(0, 0)
    for level in range(4):
        pl.semaphore_signal(ready.at[level, 0], inc=1, device_id=device(z_peers[1], my, mx, mc), device_id_type=MESH)
        pl.semaphore_signal(ready.at[level, 1], inc=1, device_id=device(z_peers[7], my, mx, mc), device_id_type=MESH)
        distances = (level + 1, NZ - level - 1) if level < 3 else (4,)
        for dz in distances:
            send_rows(dz)
            if level == 0:
                send_columns(0, dz, 2)
            if level == 1:
                send_columns(0, dz, 1)
        if level == 3:
            wait_bytes(ccx.at[0, pl.ds(0, 2)], small_recv.at[1])
            for origin, dz in ((6, 2), (6, 1), (2, 7)):
                send_columns(origin, dz, 2)
        pl.semaphore_wait(ready.at[level, 0], 1)
        pl.semaphore_wait(ready.at[level, 1], 1)
        for dz in distances:
            send_tensor(0, dz)
    for dz in Z_ORDER:
        send_tensor(1, dz)

    for q in range(2, CHUNKS):
        for dz in Z_ORDER:
            send_tensor(q, dz)

    gates_copy.wait()
    triple_products(gates, 0, right, tops, g_low)
    triple_products(gates, 3, right, tops, g_high)
    pair_products(gates, 6, right, tops, g_x)

    own_rows.wait()
    wait_bytes(crx.at[0, pl.ds(0, NZ - 1)], small_recv.at[0])
    wait_bytes(ccx.at[0, pl.ds(0, 5)], small_recv.at[2])
    for dx in (2, 1, 3):
        there = (mz, my, x_peers[dx], mc)
        remote(crx.at[mx], crx.at[mx], x_send.at[0], x_recv.at[0], there)
        remote(ccx.at[mx], ccx.at[mx], x_send.at[1], x_recv.at[1], there)

    def closing_rows_in_order():
        row = lax.broadcasted_iota(jnp.int32, (128, 2 * C), 0)
        column = lax.broadcasted_iota(jnp.int32, (128, 2 * C), 1)
        wanted = (row // KR) * 2 * KR + lax.rem(row, KR)
        wanted = jnp.where(column < C, wanted, wanted + C + KR)
        select = jnp.where(column == wanted, 1.0, 0.0).astype(BF16)
        for z in range(NZ):
            rows = [crx[xs, z, part] for part in range(2) for xs in range(NX)]
            out = jnp.dot(jnp.concatenate(rows, axis=0), select, preferred_element_type=F32)
            half = NX * AMP
            for_re = out[:half, :C] - out[half:, C:]
            for_im = out[half:, :C] + out[:half, C:]
            left[z] = jnp.concatenate([for_re, for_im], axis=0).astype(BF16)

    def columns_through_x():
        m0, m1 = lax.rem(mx, 2), mx // 2
        for xs in range(NX):
            parts = []
            for z in range(NZ):
                both = ccx[xs, z]
                parts.append(jnp.concatenate([both[0], -both[1]], axis=1))
            vectors = jnp.concatenate(parts, axis=0)
            s0, s1 = xs % 2, xs // 2
            e0 = s0 + m0 - 2 * s0 * m0
            e1 = s1 + m1 - 2 * s1 * m1
            f0 = (1 - 2 * e0).astype(F32)
            f1 = (1 - 2 * e1).astype(F32)
            cos, sin = unit(m0 + m1 - s0 - s1 - h_ones + 8)
            total = None
            for t in range(4):
                u = lax.dot_general(vectors, g_x[t], (((1,), (1,)), ((), ())), preferred_element_type=F32)
                if t & 1:
                    u = u * f0
                if t & 2:
                    u = u * f1
                total = u if total is None else total + u
            re, neg = total[:, :C], total[:, C:]
            re, neg = cos * re + sin * neg, cos * neg - sin * re
            for z in range(NZ):
                a, b = re[z * AMP : (z + 1) * AMP], neg[z * AMP : (z + 1) * AMP]
                a, b = ((a, b), (-b, a), (-a, -b), (b, -a))[ones(z)]
                wbuf[z, xs * AMP : (xs + 1) * AMP, :C] = a
                wbuf[z, xs * AMP : (xs + 1) * AMP, C:] = b

    for q in range(CHUNKS):
        wait_bytes(recv.at[q, pl.ds(0, GROUP - 1)], main_recv.at[q])

        def send_back(half):
            part = pl.ds(half * NZ // 2, NZ // 2)
            for dy, dc in back:
                py, pc = y_peers[dy], c_peers[dc]
                source = ret_send.at[q, bits_index(py, pc), part]
                remote(source, ret.at[q, mh, part], back_send.at[q], back_recv.at[q], (mz, py, mx, pc))

        sections(q, recv, work1, work2, g_low, g_high, ret_send, send_back)
        ret[q, mh] = ret_send[q, mh]

    wait_bytes(crx.at[pl.ds(0, NX - 1)], x_recv.at[0])
    wait_bytes(ccx.at[pl.ds(0, NX - 1)], x_recv.at[1])
    closing_rows_in_order()
    columns_through_x()

    for q in range(CHUNKS):
        wait_bytes(ret.at[q, pl.ds(0, NH - 1)], back_recv.at[q])

    def close(z, carry):
        blocks = []
        for h in range(NH):
            for q in range(CHUNKS):
                blocks.append(ret[q, h, z].astype(F32))
        tensor = jnp.concatenate(blocks, axis=0).astype(BF16)
        proj = jnp.dot(left[z], tensor, preferred_element_type=F32)
        half = NX * AMP
        p_re, p_im = proj[:half], proj[half:]
        w = wbuf[z]
        w_re, w_neg = w[:, :C], w[:, C:]
        a_re = p_re * w_re + p_im * w_neg
        a_im = p_im * w_re - p_re * w_neg
        both = jnp.concatenate([a_re[:, :128] + a_re[:, 128:], a_im[:, :128] + a_im[:, 128:]], axis=0)
        finz[mz, pl.ds(z, 1)] = jnp.sum(jnp.transpose(both), axis=0, keepdims=True)
        return carry

    lax.fori_loop(0, NZ, close, 0, unroll=UNROLL)

    for dz in Z_ORDER[:-1]:
        remote(finz.at[mz], finz.at[mz], fin_send.at[0], fin_recv.at[0], (z_peers[dz], my, mx, mc))
    wait_bytes(crx.at[0, pl.ds(0, NZ - 1)], small_send.at[0])
    wait_bytes(ccx.at[0, pl.ds(0, 2)], small_send.at[1])
    wait_bytes(ccx.at[0, pl.ds(0, 5)], small_send.at[2])
    wait_bytes(crx.at[pl.ds(0, NX - 1)], x_send.at[0])
    wait_bytes(ccx.at[pl.ds(0, NX - 1)], x_send.at[1])
    for q in range(CHUNKS):
        wait_bytes(recv.at[q, pl.ds(0, GROUP - 1)], main_send.at[q])
        wait_bytes(ret.at[q, pl.ds(0, NH - 1)], back_send.at[q])
    wait_bytes(finz.at[pl.ds(0, NZ - 1)], fin_recv.at[0])
    finx[mx * NH + mh] = jnp.sum(finz[...], axis=0)
    for dx, dy, dc in crossing:
        there = (mz, y_peers[dy], x_peers[dx], c_peers[dc])
        remote(finx.at[mx * NH + mh], finx.at[mx * NH + mh], fin_send.at[1], fin_recv.at[1], there)
    wait_bytes(finz.at[pl.ds(0, NZ - 1)], fin_send.at[0])
    wait_bytes(finx.at[pl.ds(0, NX * NH - 1)], fin_recv.at[1])
    finh[...] = jnp.sum(finx[...].reshape(NX, NH, NZ, 128), axis=0)
    assemble(finh, out_ref)
    wait_bytes(finx.at[pl.ds(0, NX * NH - 1)], fin_send.at[1])


def local(tensors, gates, closing_rows, closing_columns):
    dma = pltpu.SemaphoreType.DMA
    out = pl.pallas_call(
        kernel,
        out_shape=jax.ShapeDtypeStruct((2, NZ * NH * NX * AMP), F32),
        in_specs=[pl.BlockSpec(memory_space=pl.ANY)] * 4,
        out_specs=pl.BlockSpec(memory_space=pltpu.VMEM),
        scratch_shapes=[
            pltpu.VMEM((2, GROUP, 16, C), BF16),
            pltpu.VMEM((CHUNKS, GROUP, 2 * KR, C), BF16),
            pltpu.VMEM((CHUNKS, GROUP, 2 * KR, C), BF16),
            pltpu.VMEM((NH, NZ, 2 * KR, C), F32),
            pltpu.VMEM((NH, NZ, 2 * KR, C), F32),
            pltpu.VMEM((CHUNKS, NH, NZ, 2 * KR, C), BF16),
            pltpu.VMEM((CHUNKS, NH, NZ, 2 * KR, C), BF16),
            pltpu.VMEM((8, 2, 2, C, C), BF16),
            pltpu.VMEM((2, 2 * C, 2 * C), BF16),
            pltpu.VMEM((6, C, 2 * C), BF16),
            pltpu.VMEM((8, C, 2 * C), BF16),
            pltpu.VMEM((8, C, 2 * C), BF16),
            pltpu.VMEM((4, 2 * C, 2 * C), BF16),
            pltpu.VMEM((2, AMP, C), F32),
            pltpu.VMEM((NX, NZ, 2, AMP, 128), BF16),
            pltpu.VMEM((NX, NZ, 2, AMP, C), BF16),
            pltpu.VMEM((NZ, 128, C), BF16),
            pltpu.VMEM((NZ, NX * AMP, 2 * C), F32),
            pltpu.VMEM((NZ, NZ, 128), F32),
            pltpu.VMEM((NX * NH, NZ, 128), F32),
            pltpu.VMEM((NH, NZ, 128), F32),
            dma((4,)),
            dma((CHUNKS,)),
            dma((CHUNKS,)),
            dma((3,)),
            dma((3,)),
            dma((2,)),
            dma((2,)),
            dma((CHUNKS,)),
            dma((CHUNKS,)),
            dma((2,)),
            dma((2,)),
            pltpu.SemaphoreType.REGULAR((4, 2)),
        ],
        compiler_params=pltpu.CompilerParams(
            collective_id=0, has_side_effects=True, vmem_limit_bytes=56 * 1024 * 1024
        ),
        name="network",
    )(tensors.reshape(2, GROUP, 16, C), gates, closing_rows, closing_columns)
    return out * (1.0 / NX)


def solution(mesh):
    placed = (
        P(None, "sx", "sy", None, None),
        P(),
        P(None, ("sx", "sy"), None),
        P(None, ("sx", "sy"), None),
    )
    return jax.shard_map(local, mesh=mesh, in_specs=placed, out_specs=P(), check_vma=False)
```
